32 devices in a mesh: rep: 8 (over y, x, core), shard: 4 (over z).
Axes of the slice: x: 2, y: 2, z: 4, core: 2. Of those that a mesh axis runs over, the one named last changes fastest.
Arguments:
- activations: bfloat16 [6, 4096, 2048], P(None, ('rep', 'shard')), may hold values from -50 to 50
- cotangents: bfloat16 [6, 4096, 512], P(None, ('rep', 'shard')), may hold values from -120 to 120
- momentum: float32 [12, 256, 2048], P(None, None, 'shard'), may hold values from -6 to 6
- owners: int32 [12], replicated, may hold values from 0 to 3, as said below
- bucket_starts: int32 [2], replicated, may hold values from 1 to 11, as said below
Outputs:
- momentum_out: float32 [12, 256, 2048], P(None, None, 'shard')
- update: float32 [12, 256, 2048], P(None, None, 'shard')
- owned: bfloat16 [16, 256, 2048], P('shard')
The draws below stay inside these ranges and needn't reach their ends.
Inputs may be any that keep to these rules, and one draw needn't show every extreme that they name: `owners`: no owner is named more than 4 times, and some owner exactly 4 times. `bucket_starts`: strictly increasing.
All inputs are finite; a program needn't handle non-finite values.
Results may differ from the reference program's by a relative error of at most 0.033.
Values may be sent and summed in bfloat16 or wider, within the bound.
No kernel may reach another device: no remote copies, remote signals or barrier semaphores. Data moves between devices by JAX's collectives and lax.ppermute only.
A program may use at most 128 MiB of HBM per device.

```python
import math
import jax
import jax.numpy as jnp
from jax import lax

D = 2048
KV = 256
LAYERS = 6
ITERS = 5
BUCKETS = 3
MATS = 12
SLOTS = 4
TOKENS = 4096
N_SHARD = 4


def bucket_layout(key):
    key_starts = jax.random.fold_in(key, 31)
    chosen = jax.random.permutation(key_starts, MATS - 2)[:BUCKETS - 2] + 1
    last_start = jnp.full((1,), MATS - 1, dtype=jnp.int32)
    return jnp.sort(jnp.concatenate([chosen.astype(jnp.int32), last_start])).astype(jnp.int32)


def draw_activations(key, part):
    key_values = jax.random.fold_in(key, 41)
    shape_full = (LAYERS, TOKENS, D)
    values = jnp.clip(jax.random.normal(key_values, shape_full, jnp.float32), -4.5, 4.5)
    ratio = 6.0
    position = jnp.arange(D, dtype=jnp.float32) / D
    rising = jnp.exp(math.log(ratio) * position)
    mean_energy = (ratio * ratio - 1.0) / (2.0 * math.log(ratio))
    column_scale = rising / math.sqrt(mean_energy)
    return (values * column_scale[None, None, :]).astype(jnp.bfloat16)


def draw_cotangents(key, part):
    key_normal = jax.random.fold_in(key, 11)
    key_quiet_scale = jax.random.fold_in(key, 12)
    key_column = jax.random.fold_in(key, 13)
    key_quiet = jax.random.fold_in(key, 14)
    key_loud_scale = jax.random.fold_in(key, 15)
    shape_full = (LAYERS, TOKENS, 2 * KV)
    normal_part = jnp.clip(jax.random.normal(key_normal, shape_full, jnp.float32), -5.0, 5.0)
    starts = bucket_layout(key)
    indices = jnp.arange(MATS, dtype=jnp.int32)
    buckets = jnp.sum((indices[:, None] >= starts[None, :]).astype(jnp.int32), axis=1)
    quiet_bucket = jax.random.randint(key_quiet, (), 0, BUCKETS, dtype=jnp.int32)
    quiet_log = jax.random.uniform(key_quiet_scale, (MATS,), jnp.float32, math.log(0.03), math.log(0.1))
    loud_log = jax.random.uniform(key_loud_scale, (MATS,), jnp.float32, 0.0, math.log(8.0))
    matrix_scale = jnp.exp(jnp.where(buckets == quiet_bucket, quiet_log, loud_log))
    matrix_scale = jnp.repeat(matrix_scale.reshape(LAYERS, 1, 2), KV, axis=2)
    column_scale = jnp.exp(jax.random.uniform(key_column, (LAYERS, 1, 2 * KV), jnp.float32, 0.0, math.log(3.0)))
    return (normal_part * matrix_scale * column_scale).astype(jnp.bfloat16)


def draw_owners(key, part):
    key_first = jax.random.fold_in(key, 21)
    key_second = jax.random.fold_in(key, 22)
    key_third = jax.random.fold_in(key, 23)
    shuffled = jax.random.permutation(key_first, N_SHARD).astype(jnp.int32)
    filled = jnp.full((SLOTS,), shuffled[0], dtype=jnp.int32)
    others = jax.random.permutation(key_second, jnp.repeat(shuffled[1:], SLOTS))
    candidates = jnp.concatenate([filled, others])[:MATS]
    return jax.random.permutation(key_third, candidates).astype(jnp.int32)


def draw_bucket_starts(key, part):
    return bucket_layout(key)


def block_scale(rng, shape, pieces, smallest, largest):
    level = 1.0
    for axis_at, shards_of in pieces:
        steps = jax.random.uniform(jax.random.fold_in(jax.random.fold_in(rng, 6), axis_at), (shards_of,), jnp.float32, smallest / len(pieces), largest / len(pieces))
        level = level * jnp.repeat(jnp.exp(steps), shape[axis_at] // shards_of).reshape((-1,) + (1,) * (len(shape) - 1 - axis_at))
    return level


def bell_draw(stream_key, extent, deviation, limit, shards=(), kind=jnp.bfloat16):
    drawn = jax.random.normal(stream_key, extent, jnp.float32) * deviation
    if len(shards) > 0:
        drawn = block_scale(stream_key, extent, shards, -0.22, 0.18) * drawn
    return jnp.clip(drawn, min=-limit, max=limit).astype(kind)


def setup_inputs(seed: int = 0) -> dict:
    key_list = jax.random.split(jax.random.key(seed), 6)
    activations = draw_activations(jax.random.fold_in(key_list[5], 71), 0)
    cotangents = draw_cotangents(jax.random.fold_in(key_list[5], 71), 0)
    momentum = bell_draw(key_list[2], (MATS, KV, D), 1.0, 6.0, ((2, 4),), jnp.float32)
    owners = draw_owners(jax.random.fold_in(key_list[5], 71), 0)
    bucket_starts = draw_bucket_starts(jax.random.fold_in(key_list[5], 71), 0)
    return {"activations": activations, "cotangents": cotangents, "momentum": momentum, "owners": owners, "bucket_starts": bucket_starts}


coef_a = 3.4445
coef_b = -4.775
coef_c = 2.0315
momentum_rate = 0.95
clip_level = 0.5
epsilon = 1e-06

def orthogonal(update_in):
    values = update_in.astype(jnp.float32)
    frobenius = jnp.sqrt(jnp.sum(values * values))
    matrix = (values / (frobenius + epsilon)).astype(jnp.bfloat16)
    for iteration in range(ITERS):
        gram_matrix = jnp.dot(matrix, matrix.T, preferred_element_type=jnp.float32).astype(jnp.bfloat16)
        square = jnp.dot(gram_matrix, gram_matrix, preferred_element_type=jnp.float32)
        mixing = (coef_b * gram_matrix.astype(jnp.float32) + coef_c * square).astype(jnp.bfloat16)
        matrix = (coef_a * matrix.astype(jnp.float32) + jnp.dot(mixing, matrix, preferred_element_type=jnp.float32)).astype(jnp.bfloat16)
    return matrix

def clip_factors(square_sums, bucket_starts):
    indices = jnp.arange(MATS, dtype=jnp.int32)
    buckets = lax.optimization_barrier(jnp.sum((indices[:, None] >= bucket_starts[None, :]).astype(jnp.int32), axis=1))
    together = (buckets[:, None] == buckets[None, :]).astype(jnp.float32)
    totals = lax.optimization_barrier(jnp.sum(together * square_sums[None, :], axis=1))
    members = lax.optimization_barrier(jnp.sum(together, axis=1))
    root_mean = jnp.sqrt(totals / (members * KV * D) + epsilon)
    return jnp.minimum(1.0, clip_level / root_mean)

def slot_numbers(owners):
    indices = jnp.arange(MATS, dtype=jnp.int32)
    earlier = (indices[None, :] < indices[:, None]) & (owners[None, :] == owners[:, None])
    return lax.optimization_barrier(jnp.sum(earlier.astype(jnp.int32), axis=1)).astype(jnp.int32)

def reference(activations, cotangents, momentum, owners, bucket_starts):
    layer_grads = []
    for layer_index in range(LAYERS):
        layer_grads.append(lax.dot_general(cotangents[layer_index], activations[layer_index], (((0,), (0,)), ((), ())), preferred_element_type=jnp.float32))
    gradient = jnp.stack(layer_grads).reshape(MATS, KV, D) / jnp.sqrt(jnp.float32(TOKENS))
    square_sums = lax.optimization_barrier(jnp.sum(gradient * gradient, axis=(1, 2)))
    factors = clip_factors(square_sums, bucket_starts)
    momentum_out = momentum_rate * momentum + factors[:, None, None] * gradient
    nesterov = (factors[:, None, None] * gradient + momentum_rate * momentum_out).astype(jnp.bfloat16)
    orthogonalized = lax.map(orthogonal, nesterov)
    update_scale = math.sqrt(max(KV, D))
    update = update_scale * orthogonalized.astype(jnp.float32)
    slot_of = slot_numbers(owners)
    positions = owners * SLOTS + slot_of
    select = (jnp.arange(N_SHARD * SLOTS, dtype=jnp.int32)[:, None] == positions[None, :]).astype(jnp.float32)
    holdings = jnp.einsum('pm,mkd->pkd', select, update).astype(jnp.bfloat16)
    return (momentum_out, update, holdings)
```

```python
import functools
import math

import jax
import jax.numpy as jnp
from jax import lax
from jax.experimental import pallas as pl
from jax.experimental.pallas import tpu as pltpu
from jax.sharding import PartitionSpec as P

ITERS = 5

coef_a = 3.4445
coef_b = -4.775
coef_c = 2.0315
momentum_rate = 0.95
clip_level = 0.5
epsilon = 1e-06

F32 = jnp.float32
BF16 = jnp.bfloat16
NT = (((1,), (1,)), ((), ()))
NN = (((1,), (0,)), ((), ()))
TN = (((0,), (0,)), ((), ()))

CORE, BIT_X, BIT_Y = 1, 2, 4
CHIPS = 4
GROUPS = 3


def dot(a, b, dims):
    return lax.dot_general(a, b, dims, preferred_element_type=F32)


def swap_rep(value, bit):
    count = lax.axis_size("rep")
    return lax.ppermute(value, "rep", [(i, i ^ bit) for i in range(count)])


def swap_shard(value, bit, wanted=lambda source, target: True):
    count = lax.axis_size("shard")
    pairs = [(i, i ^ bit) for i in range(count) if wanted(i, i ^ bit)]
    return lax.ppermute(value, "shard", pairs)


def pick(value, index, axis=0):
    return lax.dynamic_index_in_dim(value, index, axis, keepdims=False)


def add(a, b):
    return (a.astype(F32) + b.astype(F32)).astype(BF16)


def tree_sum(values):
    while len(values) > 1:
        values = [values[i] + values[i + 1] for i in range(0, len(values), 2)]
    return values[0]


def gradient_kernel(where_ref, act, sib_act, got_act, fwd_act, cot_k, cot_v, sib_k, sib_v,
                    got_k, got_v, fwd_k, fwd_v, out):
    values = jnp.concatenate([act[0], sib_act[0], got_act[...], fwd_act[...]], axis=0)
    for kind, parts in enumerate(
        ((cot_k[0], sib_k[0], got_k[...], fwd_k[...]), (cot_v[0], sib_v[0], got_v[...], fwd_v[...]))
    ):
        terms = jnp.concatenate(parts, axis=0)
        out[kind, 0] = dot(terms, values, TN).astype(BF16)


def layer_gradient(layer, core, act, sib_act, got_act, fwd_act, cot, sib_cot, got_cot, fwd_cot, blocks):
    tokens, width = got_act.shape
    columns = width // blocks
    half = got_cot.shape[1] // 4
    whole = pl.BlockSpec((1, tokens, columns), lambda b, w: (w[0], 0, b))
    part = pl.BlockSpec((tokens, columns), lambda b, w: (0, b))
    cots = [
        pl.BlockSpec((1, tokens, half), lambda b, w, k=k: (w[0], 0, 2 * k + w[1])) for k in range(2)
    ]
    cot_parts = [pl.BlockSpec((tokens, half), lambda b, w, k=k: (0, 2 * k + w[1])) for k in range(2)]
    return pl.pallas_call(
        gradient_kernel,
        grid_spec=pltpu.PrefetchScalarGridSpec(
            num_scalar_prefetch=1,
            grid=(blocks,),
            in_specs=[whole, whole, part, part] + cots + cots + cot_parts + cot_parts,
            out_specs=pl.BlockSpec((2, 1, half, columns), lambda b, w: (0, b, 0, 0)),
        ),
        out_shape=jax.ShapeDtypeStruct((2, blocks, half, columns), BF16),
        cost_estimate=pl.CostEstimate(
            flops=2 * 4 * tokens * 2 * half * width, bytes_accessed=12 * tokens * width, transcendentals=0
        ),
        name="layer_gradient",
    )(jnp.stack([layer, core]), act, sib_act, got_act, fwd_act, cot, cot, sib_cot, sib_cot,
      got_cot, got_cot, fwd_cot, fwd_cot)


def momentum_kernel(chip_ref, unit_ref, core_ref, factor_ref, own, sib, momentum, momentum_out, nesterov):
    core = core_ref[0]
    factor = factor_ref[pl.program_id(0)]
    half = own.shape[2]
    for part, ref in ((core, own), (1 - core, sib)):
        rows = pl.ds(pl.multiple_of(part * half, half), half)
        step = factor * ref[0, 0].astype(F32)
        fresh = momentum_rate * momentum[0, rows, :] + step
        momentum_out[0, rows, :] = fresh
        nesterov[0, rows, :] = (step + momentum_rate * fresh).astype(BF16)


def momentum_step(chip, unit, core, factors, own, sib, momentum):
    mats, rows, columns = momentum.shape
    half = own.shape[2]
    piece = pl.BlockSpec((1, 1, half, columns), lambda m, c, u, k, f: (c[m], u[m], 0, 0))
    whole = pl.BlockSpec((1, rows, columns), lambda m, c, u, k, f: (m, 0, 0))
    return pl.pallas_call(
        momentum_kernel,
        grid_spec=pltpu.PrefetchScalarGridSpec(
            num_scalar_prefetch=4, grid=(mats,), in_specs=[piece, piece, whole], out_specs=[whole, whole]
        ),
        out_shape=[
            jax.ShapeDtypeStruct(momentum.shape, F32),
            jax.ShapeDtypeStruct(momentum.shape, BF16),
        ],
        cost_estimate=pl.CostEstimate(
            flops=mats * rows * columns * 400, bytes_accessed=12 * mats * rows * columns, transcendentals=0
        ),
        name="momentum_step",
    )(chip, unit, core, factors, own, sib, momentum)


def newton_kernel(core_ref, own, sib, out, x, mix):
    core = core_ref[0]
    parts, half, columns = own.shape
    spans = [slice(p * columns, (p + 1) * columns) for p in range(parts)]
    for part, ref in ((core, own), (1 - core, sib)):
        rows = pl.ds(pl.multiple_of(part * half, half), half)
        for p, span in enumerate(spans):
            x[rows, span] = ref[p]
    total = jnp.zeros((), F32)
    for span in spans:
        values = x[:, span].astype(F32)
        total = total + jnp.sum(values * values)
    inverse = 1.0 / (jnp.sqrt(jnp.full((1, 1), total, F32)) + epsilon)
    for span in spans:
        x[:, span] = (x[:, span].astype(F32) * inverse).astype(BF16)
    size = 2 * half
    diagonal = lax.broadcasted_iota(jnp.int32, (size, size), 0) == lax.broadcasted_iota(
        jnp.int32, (size, size), 1
    )
    for iteration in range(ITERS):
        gram = dot(x[...], x[...], NT).astype(BF16)
        square = dot(gram, gram, NN)
        mixing = (coef_b * gram.astype(F32) + coef_c * square).astype(BF16)
        if iteration < ITERS - 1:
            for span in spans:
                block = x[:, span]
                x[:, span] = (coef_a * block.astype(F32) + dot(mixing, block, NN)).astype(BF16)
        if iteration == 0:
            mix[...] = jnp.where(diagonal, coef_a, 0.0) + mixing.astype(F32)
        else:
            product = mix[...]
            high = product.astype(BF16)
            low = (product - high.astype(F32)).astype(BF16)
            mix[...] = coef_a * product + (dot(mixing, high, NN) + dot(mixing, low, NN))
    out[...] = mix[pl.ds(pl.multiple_of(core * half, half), half), :] * inverse


def newton(core, own, sib):
    parts, half, columns = own.shape
    size = 2 * half
    return pl.pallas_call(
        newton_kernel,
        grid_spec=pltpu.PrefetchScalarGridSpec(
            num_scalar_prefetch=1,
            grid=(1,),
            in_specs=[pl.BlockSpec(own.shape, lambda i, c: (0, 0, 0))] * 2,
            out_specs=pl.BlockSpec((half, size), lambda i, c: (0, 0)),
            scratch_shapes=[pltpu.VMEM((size, parts * columns), BF16), pltpu.VMEM((size, size), F32)],
        ),
        out_shape=jax.ShapeDtypeStruct((half, size), F32),
        cost_estimate=pl.CostEstimate(
            flops=ITERS * 2 * size * size * (2 * parts * columns + 3 * size),
            bytes_accessed=4 * size * parts * columns, transcendentals=0,
        ),
        name="newton",
    )(core, own, sib)


def apply_rows(matrix, values):
    high = matrix.astype(BF16)
    low = (matrix - high.astype(F32)).astype(BF16)
    return (dot(high, values, NN) + dot(low, values, NN)).astype(BF16)


def update_kernel(scale, chip_ref, unit_ref, core_ref, own, sib, values, out):
    core = core_ref[0]
    half = own.shape[2]
    for part, ref in ((core, own), (1 - core, sib)):
        rows = pl.ds(pl.multiple_of(part * half, half), half)
        out[0, rows, :] = scale * apply_rows(ref[0, 0], values[0]).astype(F32)


def update_step(scale, chip, unit, core, own, sib, values):
    mats, rows, columns = values.shape
    half = own.shape[2]
    piece = pl.BlockSpec((1, 1, half, rows), lambda m, c, u, k: (c[m], u[m], 0, 0))
    whole = pl.BlockSpec((1, rows, columns), lambda m, c, u, k: (m, 0, 0))
    return pl.pallas_call(
        functools.partial(update_kernel, scale),
        grid_spec=pltpu.PrefetchScalarGridSpec(
            num_scalar_prefetch=3, grid=(mats,), in_specs=[piece, piece, whole], out_specs=whole
        ),
        out_shape=jax.ShapeDtypeStruct(values.shape, F32),
        cost_estimate=pl.CostEstimate(
            flops=4 * mats * rows * rows * columns, bytes_accessed=8 * mats * rows * columns, transcendentals=0
        ),
        name="update_step",
    )(chip, unit, core, own, sib, values)


def owned_kernel(scale, chip_ref, unit_ref, filled_ref, held_ref, place_ref, core_ref, own, sib,
                 own_rows, sib_rows, out, values):
    core = core_ref[0]
    half = own.shape[2]
    for part, ref in ((core, own_rows), (1 - core, sib_rows)):
        values[pl.ds(pl.multiple_of(part * half, half), half), :] = ref[0, 0]
    filled = filled_ref[pl.program_id(0)] > 0
    for part, ref in ((core, own), (1 - core, sib)):
        rows = pl.ds(pl.multiple_of(part * half, half), half)
        result = (scale * apply_rows(ref[0, 0], values[...]).astype(F32)).astype(BF16)
        out[0, rows, :] = jnp.where(filled, result, jnp.zeros_like(result))


def owned_step(scale, chip, unit, filled, held, place, core, own, sib, own_rows, sib_rows):
    slots, blocks, half, columns = own_rows.shape
    rows = 2 * half
    piece = pl.BlockSpec((1, 1, half, rows), lambda p, b, c, u, f, h, t, k: (c[p], u[p], 0, 0))
    block = pl.BlockSpec((1, 1, half, columns), lambda p, b, c, u, f, h, t, k: (h[p], t[b], 0, 0))
    return pl.pallas_call(
        functools.partial(owned_kernel, scale),
        grid_spec=pltpu.PrefetchScalarGridSpec(
            num_scalar_prefetch=6,
            grid=(slots, blocks),
            in_specs=[piece, piece, block, block],
            out_specs=pl.BlockSpec((1, rows, columns), lambda p, b, c, u, f, h, t, k: (p, 0, b)),
            scratch_shapes=[pltpu.VMEM((rows, columns), BF16)],
        ),
        out_shape=jax.ShapeDtypeStruct((slots, rows, blocks * columns), BF16),
        cost_estimate=pl.CostEstimate(
            flops=4 * slots * rows * rows * blocks * columns,
            bytes_accessed=4 * slots * rows * blocks * columns, transcendentals=0,
        ),
        name="owned_step",
    )(chip, unit, filled, held, place, core, own, sib, own_rows, sib_rows)


def clip_factors(square_sums, bucket_starts, elements):
    mats = square_sums.shape[0]
    indices = jnp.arange(mats, dtype=jnp.int32)
    buckets = jnp.sum((indices[:, None] >= bucket_starts[None, :]).astype(jnp.int32), axis=1)
    together = (buckets[:, None] == buckets[None, :]).astype(F32)
    totals = jnp.sum(together * square_sums[None, :], axis=1)
    members = jnp.sum(together, axis=1)
    root_mean = jnp.sqrt(totals / (members * elements) + epsilon)
    return jnp.minimum(1.0, clip_level / root_mean)


def slot_numbers(owners):
    indices = jnp.arange(owners.shape[0], dtype=jnp.int32)
    earlier = (indices[None, :] < indices[:, None]) & (owners[None, :] == owners[:, None])
    return jnp.sum(earlier.astype(jnp.int32), axis=1)


def over_chips(value):
    return jnp.stack([value] + [swap_rep(value, BIT_X * k) for k in range(1, CHIPS)])


def per_device(activations, cotangents, momentum, owners, bucket_starts):
    shard_count = lax.axis_size("shard")
    replica_count = lax.axis_size("rep")
    shard = lax.axis_index("shard")
    replica = lax.axis_index("rep")
    layers, tokens, width = activations.shape
    mats, rows, columns = momentum.shape
    half = rows // 2
    token_total = tokens * shard_count * replica_count
    slot_count = -(-mats // shard_count) + 1
    update_scale = math.sqrt(max(rows, width))
    core = replica & 1
    bit_x = (replica >> 1) & 1
    bit_y = (replica >> 2) & 1
    bit_z = shard & 1
    chip = (replica >> 1) & (CHIPS - 1)
    core_table = core[None]

    chosen = (bit_x, bit_y, bit_z)
    swaps = (
        lambda v: swap_rep(v, BIT_X),
        lambda v: swap_rep(v, BIT_Y),
        lambda v: swap_shard(v, 1),
    )
    got = []
    for group in range(GROUPS):
        other = 2 * group + 1 - chosen[group]
        got.append((swaps[group](pick(activations, other)), swaps[group](pick(cotangents, other))))
    sib_act = swap_rep(activations, CORE)
    sib_cot = swap_rep(cotangents, CORE)
    partial = []
    for group in range(GROUPS):
        got_act, got_cot = got[group]
        partial.append(
            layer_gradient(
                2 * group + chosen[group], core, activations, sib_act, got_act, swap_rep(got_act, CORE),
                cotangents, sib_cot, got_cot, swap_rep(got_cot, CORE), shard_count,
            )
        )
    pairs = shard_count // 2
    split = (2, pairs, 2, half, columns)
    first, second, third = partial
    second = second.reshape(split)
    first = add(pick(first, bit_y), swaps[1](pick(first, 1 - bit_y)))
    second = add(pick(second, bit_z, 2), swaps[2](pick(second, 1 - bit_z, 2)))
    third = add(pick(third, bit_x), swaps[0](pick(third, 1 - bit_x)))
    first = first.reshape(split[1:])
    third = third.reshape(split[1:])
    first = add(pick(first, bit_z, 1), swaps[2](pick(first, 1 - bit_z, 1)))
    second = add(pick(second, bit_x), swaps[0](pick(second, 1 - bit_x)))
    third = add(pick(third, bit_y, 1), swaps[1](pick(third, 1 - bit_y, 1)))
    terms = jnp.stack([first, second, third])
    bit = 2
    while bit < shard_count:
        low = (shard // bit) & 1
        terms = terms.reshape(GROUPS, -1, 2, half, columns)
        terms = add(pick(terms, low, 2), swap_shard(pick(terms, 1 - low, 2), bit))
        bit *= 2
    terms = terms.reshape(GROUPS, half, columns)
    bit = BIT_Y * 2
    while bit < replica_count:
        terms = add(terms, swap_rep(terms, bit))
        bit *= 2
    turned = [
        (r * shard_count + s, (r ^ BIT_Y) * shard_count + (s ^ 1))
        for r in range(replica_count)
        for s in range(shard_count)
        if ((r // BIT_Y) & 1) != (s & 1)
    ]
    moved = lax.ppermute(terms[2], ("rep", "shard"), turned)
    last = jnp.where(bit_y == bit_z, terms[2], moved)
    gradient = jnp.concatenate([terms[:2], last[None]])
    inverse = 1.0 / math.sqrt(token_total)
    gradient = (gradient.astype(F32) * inverse).astype(BF16)

    table_chip = []
    table_unit = []
    for matrix in range(mats):
        unit, place = divmod(matrix, CHIPS)
        table_unit.append(unit)
        table_chip.append(2 * (place & 1) + (place >> 1) if unit == 0 else place)
    unit_of = jnp.array(table_unit, jnp.int32)
    chip_of = jnp.array(table_chip, jnp.int32) ^ chip
    mine = jnp.stack([2 * bit_x + bit_y, CHIPS + chip, 2 * CHIPS + chip])

    all_gradient = over_chips(gradient)
    all_gradient_sib = swap_rep(all_gradient, CORE)

    wide = gradient.astype(F32)
    sums = jnp.sum(wide * wide, axis=(1, 2))
    placed = (jnp.arange(mats, dtype=jnp.int32)[None, :] == mine[:, None]).astype(F32)
    sums = jnp.sum(placed * sums[:, None], axis=0)
    sums = tree_sum([sums] + [swap_rep(sums, k) for k in range(1, 2 * CHIPS)])
    sums = tree_sum([sums] + [swap_shard(sums, k) for k in range(1, shard_count)])
    factors = clip_factors(sums, bucket_starts, rows * width)

    own_inputs = []
    split_momentum = momentum.reshape(mats, 2, half, columns)
    for unit in range(GROUPS):
        step = pick(factors, mine[unit]) * wide[unit]
        before = lax.dynamic_slice(
            split_momentum, (mine[unit], core, 0, 0), (1, 1, half, columns)
        ).reshape(half, columns)
        own_inputs.append((step + momentum_rate * (momentum_rate * before + step)).astype(BF16))
    own_inputs = jnp.stack(own_inputs)
    slices = [pick(own_inputs, jnp.minimum(shard, GROUPS - 1))]
    for k in range(1, shard_count):
        slices.append(
            swap_shard(
                pick(own_inputs, jnp.minimum(shard ^ k, GROUPS - 1)), k,
                lambda source, target: target < GROUPS,
            )
        )
    whole = jnp.stack(slices)
    mixing = newton(core_table, whole, swap_rep(whole, CORE))
    products = [mixing] + [
        swap_shard(mixing, k, lambda source, target: source < GROUPS) for k in range(1, shard_count)
    ]
    products = jnp.stack(products)
    products = jnp.stack([pick(products, shard ^ unit) for unit in range(GROUPS)])
    all_products = over_chips(products)
    all_products_sib = swap_rep(all_products, CORE)

    momentum_out, nesterov = momentum_step(
        chip_of, unit_of, core_table, factors, all_gradient, all_gradient_sib, momentum
    )

    slot_of = slot_numbers(owners)
    indices = jnp.arange(mats, dtype=jnp.int32)
    holders = jnp.arange(shard_count, dtype=jnp.int32)
    places = jnp.arange(slot_count, dtype=jnp.int32)
    chosen_at = (holders[:, None, None] == owners[None, None, :]) & (
        places[None, :, None] == slot_of[None, None, :]
    )
    matrix_at = jnp.sum(jnp.where(chosen_at, indices[None, None, :], 0), axis=2)
    filled_at = jnp.sum(chosen_at.astype(jnp.int32), axis=2)
    my_place = chip % slot_count
    split_inputs = nesterov.reshape(mats, 2, half, columns)

    def carried(target):
        matrix = lax.dynamic_slice(matrix_at, (target, my_place), (1, 1))[0, 0]
        return lax.dynamic_slice(
            split_inputs, (matrix, core, 0, 0), (1, 1, half, columns)
        ).reshape(half, columns)

    slot_rows = jnp.stack(
        [carried(shard)] + [swap_shard(carried(shard ^ k), k) for k in range(1, shard_count)]
    )
    slot_rows = jnp.stack([slot_rows] + [swap_rep(slot_rows, BIT_X * k) for k in range(1, slot_count)])
    slot_rows_sib = swap_rep(slot_rows, CORE)

    update = update_step(
        update_scale, chip_of, unit_of, core_table, all_products, all_products_sib, nesterov
    )
    my_matrices = pick(matrix_at, shard)
    owned = owned_step(
        update_scale, chip_of[my_matrices], unit_of[my_matrices], pick(filled_at, shard),
        places ^ my_place, holders ^ shard, core_table, all_products, all_products_sib,
        slot_rows, slot_rows_sib,
    )
    return (momentum_out, update, owned)


def solution(mesh):
    placed = (
        P(None, ("rep", "shard"), None),
        P(None, ("rep", "shard"), None),
        P(None, None, "shard"),
        P(),
        P(),
    )
    return jax.shard_map(
        per_device,
        mesh=mesh,
        in_specs=placed,
        out_specs=(P(None, None, "shard"), P(None, None, "shard"), P("shard", None, None)),
        check_vma=False,
    )
```

```python
import functools
import math

import jax
import jax.numpy as jnp
from jax import lax
from jax.experimental import pallas as pl
from jax.experimental.pallas import tpu as pltpu
from jax.sharding import PartitionSpec as P

ITERS = 5

coef_a = 3.4445
coef_b = -4.775
coef_c = 2.0315
momentum_rate = 0.95
clip_level = 0.5
epsilon = 1e-06


F32 = jnp.float32
BF16 = jnp.bfloat16
NT = (((1,), (1,)), ((), ()))
NN = (((1,), (0,)), ((), ()))

CORE, BIT_X, BIT_Y = 1, 2, 4
CHIPS = 4
GROUPS = 3


def dot(a, b, dims):
    return lax.dot_general(a, b, dims, preferred_element_type=F32)


def swap_rep(value, bit):
    count = lax.axis_size("rep")
    return lax.ppermute(value, "rep", [(i, i ^ bit) for i in range(count)])


def swap_shard(value, bit, wanted=lambda source, target: True):
    count = lax.axis_size("shard")
    pairs = [(i, i ^ bit) for i in range(count) if wanted(i, i ^ bit)]
    return lax.ppermute(value, "shard", pairs)


def pick(value, index, axis=0):
    return lax.dynamic_index_in_dim(value, index, axis, keepdims=False)


def add(a, b):
    return (a.astype(F32) + b.astype(F32)).astype(BF16)


VMEM = pl.BlockSpec(memory_space=pltpu.VMEM)
ANY = pl.BlockSpec(memory_space=pl.ANY)
SMEM = pl.BlockSpec(memory_space=pltpu.SMEM)

AT_CORE, AT_X, AT_Y, AT_Z, AT_CHIP, AT_SHARD, AT_PLACE, AT_LOW, AT_LISTS = range(9)


def unit_of(matrix):
    return matrix // CHIPS


def chip_of(matrix):
    place = matrix % CHIPS
    turned = 2 * (place % 2) + place // 2
    if isinstance(matrix, int):
        return turned if matrix < CHIPS else place
    return jnp.where(matrix < CHIPS, turned, place)


def matrix_of(table, unit):
    chip = table[AT_CHIP]
    if isinstance(unit, int):
        return CHIPS * unit + chip if unit else 2 * table[AT_X] + table[AT_Y]
    return jnp.where(unit == 0, 2 * table[AT_X] + table[AT_Y], CHIPS * unit + chip)


def load_kernel(table, activations, cotangents, *rest):
    outs, sems = rest[:-1], rest[-1]
    width = activations.shape[2]
    copies = []
    for group, out in enumerate(outs):
        layer = table[group]
        copies.append(
            pltpu.make_async_copy(activations.at[layer], out.at[:, :width], sems.at[2 * group])
        )
        copies.append(
            pltpu.make_async_copy(cotangents.at[layer], out.at[:, width:], sems.at[2 * group + 1])
        )
    for copy in copies:
        copy.start()
    for copy in copies:
        copy.wait()


def load_layers(layers, activations, cotangents):
    _, tokens, width = activations.shape
    terms = cotangents.shape[2]
    return pl.pallas_call(
        load_kernel,
        in_specs=[SMEM, ANY, ANY],
        out_specs=[VMEM] * GROUPS,
        out_shape=[jax.ShapeDtypeStruct((tokens, width + terms), BF16)] * GROUPS,
        scratch_shapes=[pltpu.SemaphoreType.DMA((2 * GROUPS,))],
        cost_estimate=pl.CostEstimate(
            flops=GROUPS * tokens * width * 100, bytes_accessed=4 * GROUPS * tokens * (width + terms),
            transcendentals=0,
        ),
        name="load_layers",
    )(jnp.stack(layers), activations, cotangents)


def gradient_rows(table, group, width, half, sources, turned):
    for source, ref in enumerate(sources):
        tokens = ref.shape[0]
        for part in range(2):
            kind = part
            if group == 0:
                kind = 1 - table[AT_Y] if part else table[AT_Y]
            at = pl.multiple_of(width + (2 * kind + table[AT_CORE]) * half, half)
            turned[part * half:(part + 1) * half, source * tokens:(source + 1) * tokens] = ref[
                :, pl.ds(at, half)
            ].T


def local_kernel(width, blocks, table, mine0, mine1, mine2, sib0, sib1, sib2, out0, out1, out2, turned):
    half = turned.shape[1] // 2
    columns = width // blocks
    for group, (mine, sib, out) in enumerate(((mine0, sib0, out0), (mine1, sib1, out1), (mine2, sib2, out2))):
        sources = (mine, sib)
        gradient_rows(table, group, width, half, sources, turned.at[group])
        for block in range(blocks):
            span = slice(block * columns, (block + 1) * columns)
            values = jnp.concatenate([ref[:, span] for ref in sources], axis=0)
            out[:, span] = dot(turned[group], values, NN)


def gradient_kernel(group, width, blocks, table, local, got, fwd, keep, send, turned):
    half = turned.shape[0] // 2
    columns = width // blocks
    sources = (got, fwd)
    gradient_rows(table, group, width, half, sources, turned)
    for block in range(blocks):
        span = slice(block * columns, (block + 1) * columns)
        values = jnp.concatenate([ref[:, span] for ref in sources], axis=0)
        terms = (local[:, span] + dot(turned[...], values, NN)).astype(BF16)
        if group == 0:
            keep[block] = terms[:half]
            send[block] = terms[half:]
            continue
        if group == 1:
            bit, value, at = table[AT_Z], block % 2, block // 2
        else:
            bit, value, at = table[AT_LOW], block // (blocks // 2), block % (blocks // 2)

        @pl.when(bit == value)
        def _():
            keep[0, at] = terms[:half]
            keep[1, at] = terms[half:]

        @pl.when(bit != value)
        def _():
            send[0, at] = terms[:half]
            send[1, at] = terms[half:]


def local_gradients(table, mine, sib, width, blocks, half):
    tokens = mine[0].shape[0]
    return pl.pallas_call(
        functools.partial(local_kernel, width, blocks),
        in_specs=[SMEM] + [VMEM] * 6,
        out_specs=[VMEM] * GROUPS,
        out_shape=[jax.ShapeDtypeStruct((2 * half, width), F32)] * GROUPS,
        scratch_shapes=[pltpu.VMEM((GROUPS, 2 * half, 2 * tokens), BF16)],
        cost_estimate=pl.CostEstimate(
            flops=GROUPS * 2 * 2 * tokens * 2 * half * width, bytes_accessed=GROUPS * 12 * tokens * width,
            transcendentals=0,
        ),
        name="local_gradients",
    )(table, *mine, *sib)


def layer_gradient(group, table, local, got, fwd, width, blocks, half):
    columns = width // blocks
    tokens = got.shape[0]
    shape = (blocks, half, columns) if group == 0 else (2, blocks // 2, half, columns)
    return pl.pallas_call(
        functools.partial(gradient_kernel, group, width, blocks),
        in_specs=[SMEM] + [VMEM] * 3,
        out_specs=[VMEM] * 2,
        out_shape=[jax.ShapeDtypeStruct(shape, BF16)] * 2,
        scratch_shapes=[pltpu.VMEM((2 * half, 2 * tokens), BF16)],
        cost_estimate=pl.CostEstimate(
            flops=2 * 2 * tokens * 2 * half * width, bytes_accessed=12 * tokens * width, transcendentals=0
        ),
        name="layer_gradient",
    )(table, local, got, fwd)


def finish_kernel(scale, table, keep, got, keep_last, got_last, out, last, sums):
    lane = lax.broadcasted_iota(jnp.int32, sums.shape, 1)
    held = (
        matrix_of(table, 0),
        matrix_of(table, 1),
        2 * CHIPS + 2 * table[AT_Z] + table[AT_X],
    )
    total = jnp.zeros(sums.shape, F32)
    for unit in range(GROUPS):
        if unit < GROUPS - 1:
            values = keep[unit, table[AT_LOW]].astype(F32) + got[unit].astype(F32)
        else:
            values = keep_last[...].astype(F32) + got_last[...].astype(F32)
        values = (values * scale).astype(BF16)
        if unit < GROUPS - 1:
            out[unit] = values
        else:
            last[...] = values
        wide = values.astype(F32)
        total = total + jnp.where(lane == held[unit], jnp.sum(wide * wide), 0.0)
    sums[...] = total


def finish(scale, table, keep, got, keep_last, got_last):
    return pl.pallas_call(
        functools.partial(finish_kernel, scale),
        in_specs=[SMEM] + [VMEM] * 4,
        out_specs=[VMEM] * 3,
        out_shape=[
            jax.ShapeDtypeStruct(got.shape, BF16),
            jax.ShapeDtypeStruct(got_last.shape, BF16),
            jax.ShapeDtypeStruct((1, 128), F32),
        ],
        cost_estimate=pl.CostEstimate(flops=1000 * got.size, bytes_accessed=8 * got.size, transcendentals=0),
        name="finish",
    )(table, keep, got, keep_last, got_last)


def momentum_kernel(table, factors, own, sib, momentum, momentum_out, nesterov, buffer, came, left):
    core, chip = table[AT_CORE], table[AT_CHIP]
    half = own.shape[2]
    mats = buffer.shape[0]
    ins = [pltpu.make_async_copy(momentum.at[m], buffer.at[m], came.at[m]) for m in range(mats)]
    outs = [pltpu.make_async_copy(buffer.at[m], momentum_out.at[m], left.at[m]) for m in range(mats)]
    for copy in ins:
        copy.start()
    for matrix in range(mats):
        ins[matrix].wait()
        factor = factors[matrix]
        place, unit = chip_of(matrix) ^ chip, unit_of(matrix)
        for part, ref in ((core, own), (1 - core, sib)):
            rows = pl.ds(pl.multiple_of(part * half, half), half)
            step = factor * ref[place, unit].astype(F32)
            fresh = momentum_rate * buffer[matrix, rows, :] + step
            buffer[matrix, rows, :] = fresh
            nesterov[matrix, rows, :] = (step + momentum_rate * fresh).astype(BF16)
        outs[matrix].start()
    for copy in outs:
        copy.wait()


def momentum_step(table, factors, own, sib, momentum):
    mats, rows, columns = momentum.shape
    return pl.pallas_call(
        momentum_kernel,
        in_specs=[SMEM, SMEM, VMEM, VMEM, ANY],
        out_specs=[ANY, VMEM],
        out_shape=[
            jax.ShapeDtypeStruct(momentum.shape, F32),
            jax.ShapeDtypeStruct(momentum.shape, BF16),
        ],
        scratch_shapes=[
            pltpu.VMEM(momentum.shape, F32), pltpu.SemaphoreType.DMA((mats,)), pltpu.SemaphoreType.DMA((mats,))
        ],
        cost_estimate=pl.CostEstimate(
            flops=mats * rows * columns * 400, bytes_accessed=12 * mats * rows * columns, transcendentals=0
        ),
        name="momentum_step",
    )(table, factors, own, sib, momentum)


def rows_kernel(table, factors, gradient, old, *outs):
    for k, out in enumerate(outs):
        unit = jnp.minimum(table[AT_SHARD] ^ k, GROUPS - 1)
        step = factors[matrix_of(table, unit)] * gradient[unit].astype(F32)
        fresh = momentum_rate * old[unit] + step
        out[...] = (step + momentum_rate * fresh).astype(BF16)


def newton_rows(table, factors, gradient, old, shard_count):
    _, half, columns = gradient.shape
    return pl.pallas_call(
        rows_kernel,
        in_specs=[SMEM, SMEM, VMEM, VMEM],
        out_specs=[VMEM] * shard_count,
        out_shape=[jax.ShapeDtypeStruct((half, columns), BF16)] * shard_count,
        cost_estimate=pl.CostEstimate(
            flops=shard_count * half * columns * 100, bytes_accessed=8 * shard_count * half * columns,
            transcendentals=0,
        ),
        name="newton_rows",
    )(table, factors, gradient, old)


def carried_kernel(targets, table, factors, own, *rest):
    refs, outs, sems = rest[0], rest[1:-2], rest[-2:]
    buffer, sem = sems
    core, chip, shard = table[AT_CORE], table[AT_CHIP], table[AT_SHARD]
    half = own.shape[2]
    matrices = [table[AT_LISTS + (shard ^ k)] for k in targets]
    copies = []
    for i, matrix in enumerate(matrices):
        rows = pl.ds(pl.multiple_of(core * half, half), half)
        copies.append(pltpu.make_async_copy(refs.at[matrix, rows, :], buffer.at[i], sem.at[i]))
        copies[-1].start()
    for i, matrix in enumerate(matrices):
        copies[i].wait()
        step = factors[matrix] * own[chip_of(matrix) ^ chip, unit_of(matrix)].astype(F32)
        fresh = momentum_rate * buffer[i] + step
        outs[i][...] = (step + momentum_rate * fresh).astype(BF16)


def carried_rows(table, factors, own, momentum, shard_count):
    half, columns = own.shape[2:]
    targets = tuple(range(1, shard_count))
    count = len(targets)
    return pl.pallas_call(
        functools.partial(carried_kernel, targets),
        in_specs=[SMEM, SMEM, VMEM, ANY],
        out_specs=[VMEM] * count,
        out_shape=[jax.ShapeDtypeStruct((half, columns), BF16)] * count,
        scratch_shapes=[pltpu.VMEM((count, half, columns), F32), pltpu.SemaphoreType.DMA((count,))],
        cost_estimate=pl.CostEstimate(
            flops=count * half * columns * 100, bytes_accessed=8 * count * half * columns, transcendentals=0
        ),
        name="carried_rows",
    )(table, factors, own, momentum)


def newton_kernel(table, own, sib, out, x, mix):
    core = table[AT_CORE]
    parts, half, columns = own.shape
    spans = [slice(p * columns, (p + 1) * columns) for p in range(parts)]
    total = jnp.zeros((1, 1), F32)
    for part, ref in ((core, own), (1 - core, sib)):
        rows = pl.ds(pl.multiple_of(part * half, half), half)
        for p, span in enumerate(spans):
            x[rows, span] = ref[p]
            wide = ref[p].astype(F32)
            total = total + jnp.sum(wide * wide)
    inverse = 1.0 / (jnp.sqrt(total) + epsilon)
    for span in spans:
        x[:, span] = (x[:, span].astype(F32) * inverse).astype(BF16)
    size = 2 * half
    diagonal = lax.broadcasted_iota(jnp.int32, (size, size), 0) == lax.broadcasted_iota(
        jnp.int32, (size, size), 1
    )
    for iteration in range(ITERS):
        gram = dot(x[...], x[...], NT).astype(BF16)
        square = dot(gram, gram, NN)
        mixing = (coef_b * gram.astype(F32) + coef_c * square).astype(BF16)
        if iteration < ITERS - 1:
            for span in spans:
                block = x[:, span]
                x[:, span] = (coef_a * block.astype(F32) + dot(mixing, block, NN)).astype(BF16)
        if iteration == 0:
            mix[...] = jnp.where(diagonal, coef_a, 0.0) + mixing.astype(F32)
        else:
            product = mix[...]
            high = product.astype(BF16)
            low = (product - high.astype(F32)).astype(BF16)
            mix[...] = coef_a * product + (dot(mixing, high, NN) + dot(mixing, low, NN))
    out[...] = (mix[pl.ds(pl.multiple_of(core * half, half), half), :] * inverse).astype(BF16)


def newton(table, own, sib):
    parts, half, columns = own.shape
    size = 2 * half
    return pl.pallas_call(
        newton_kernel,
        in_specs=[SMEM, VMEM, VMEM],
        out_specs=VMEM,
        scratch_shapes=[pltpu.VMEM((size, parts * columns), BF16), pltpu.VMEM((size, size), F32)],
        out_shape=jax.ShapeDtypeStruct((half, size), BF16),
        cost_estimate=pl.CostEstimate(
            flops=ITERS * 2 * size * size * (2 * parts * columns + 3 * size),
            bytes_accessed=8 * size * parts * columns, transcendentals=0,
        ),
        name="newton",
    )(table, own, sib)


def gather_rows(core, own, sib, out):
    half = own.shape[0]
    for part, block in ((core, own), (1 - core, sib)):
        out[pl.ds(pl.multiple_of(part * half, half), half), :] = block


def apply_kernel(scale, first, table, own, sib, values, own_rows, sib_rows, update, owned,
                 mix, rows, whole, held, sems):
    core, chip, shard = table[AT_CORE], table[AT_CHIP], table[AT_SHARD]
    mats = values.shape[0]
    slots, others, _, columns = own_rows.shape
    copies = []

    def leave(source, target):
        copies.append(pltpu.make_async_copy(source, target, sems.at[len(copies)]))
        copies[-1].start()

    for slot in range(slots):
        matrix = table[first + slot]
        filled = table[first + slots + slot] > 0
        place, unit = chip_of(matrix) ^ chip, unit_of(matrix)
        gather_rows(core, own[place, unit], sib[place, unit], mix.at[slot])
        at = table[AT_PLACE] ^ slot
        for k in range(others + 1):
            if k == 0:
                block = values[matrix]
            else:
                gather_rows(core, own_rows[at, k - 1], sib_rows[at, k - 1], rows.at[k - 1])
                block = rows[k - 1]
            result = scale * dot(mix[slot], block, NN).astype(BF16).astype(F32)
            span = pl.ds(pl.multiple_of((shard ^ k) * columns, columns), columns)
            held[slot, :, span] = jnp.where(filled, result, 0.0).astype(BF16)
        leave(held.at[slot], owned.at[slot])
    for matrix in range(mats):
        place, unit = chip_of(matrix) ^ chip, unit_of(matrix)
        gather_rows(core, own[place, unit], sib[place, unit], mix.at[slots + matrix])
        whole[matrix] = scale * dot(mix[slots + matrix], values[matrix], NN).astype(BF16).astype(F32)
        leave(whole.at[matrix], update.at[matrix])
    for copy in copies:
        copy.wait()


def apply_step(scale, table, own, sib, values, own_rows, sib_rows, shard_count):
    mats, rows, columns = values.shape
    slots, others, _, _ = own_rows.shape
    width = (others + 1) * columns
    return pl.pallas_call(
        functools.partial(apply_kernel, scale, AT_LISTS + shard_count),
        in_specs=[SMEM] + [VMEM] * 5,
        out_specs=[ANY, ANY],
        out_shape=[
            jax.ShapeDtypeStruct(values.shape, F32),
            jax.ShapeDtypeStruct((slots, rows, width), BF16),
        ],
        scratch_shapes=[
            pltpu.VMEM((slots + mats, rows, rows), BF16),
            pltpu.VMEM((others, rows, columns), BF16),
            pltpu.VMEM(values.shape, F32),
            pltpu.VMEM((slots, rows, width), BF16),
            pltpu.SemaphoreType.DMA((slots + mats,)),
        ],
        cost_estimate=pl.CostEstimate(
            flops=2 * rows * rows * (mats * columns + slots * width),
            bytes_accessed=6 * mats * rows * columns + 2 * slots * rows * width, transcendentals=0,
        ),
        name="apply_step",
    )(table, own, sib, values, own_rows, sib_rows)


def clip_factors(square_sums, bucket_starts, elements):
    mats = square_sums.shape[0]
    indices = jnp.arange(mats, dtype=jnp.int32)
    buckets = jnp.sum((indices[:, None] >= bucket_starts[None, :]).astype(jnp.int32), axis=1)
    together = (buckets[:, None] == buckets[None, :]).astype(F32)
    totals = jnp.sum(together * square_sums[None, :], axis=1)
    members = jnp.sum(together, axis=1)
    root_mean = jnp.sqrt(totals / (members * elements) + epsilon)
    return jnp.minimum(1.0, clip_level / root_mean)


def slot_numbers(owners):
    indices = jnp.arange(owners.shape[0], dtype=jnp.int32)
    earlier = (indices[None, :] < indices[:, None]) & (owners[None, :] == owners[:, None])
    return jnp.sum(earlier.astype(jnp.int32), axis=1)


def over_chips(value):
    return jnp.stack([value] + [swap_rep(value, BIT_X * k) for k in range(1, CHIPS)])


def small_table(owners, scalars, shard, place, shard_count, slot_count):
    indices = jnp.arange(owners.shape[0], dtype=jnp.int32)
    slot_of = slot_numbers(owners)
    holders = jnp.arange(shard_count, dtype=jnp.int32)
    places = jnp.arange(slot_count, dtype=jnp.int32)
    of_place = (holders[:, None] == owners[None, :]) & (slot_of == place)[None, :]
    of_shard = (places[:, None] == slot_of[None, :]) & (owners == shard)[None, :]
    return jnp.concatenate(
        [
            jnp.stack(scalars),
            jnp.sum(jnp.where(of_place, indices[None, :], 0), axis=1),
            jnp.sum(jnp.where(of_shard, indices[None, :], 0), axis=1),
            jnp.sum(of_shard.astype(jnp.int32), axis=1),
        ]
    )


def step(activations, cotangents, momentum, owners, bucket_starts):
    shard_count = lax.axis_size("shard")
    replica_count = lax.axis_size("rep")
    shard = lax.axis_index("shard")
    replica = lax.axis_index("rep")
    _, tokens, width = activations.shape
    mats, rows, columns = momentum.shape
    half = rows // 2
    token_total = tokens * shard_count * replica_count
    slot_count = -(-mats // shard_count) + 1
    update_scale = math.sqrt(max(rows, width))
    core = replica & 1
    bit_x = (replica >> 1) & 1
    bit_y = (replica >> 2) & 1
    bit_z = shard & 1
    chip = (replica >> 1) & (CHIPS - 1)
    place = chip % slot_count
    swaps = (
        lambda v: swap_rep(v, BIT_X),
        lambda v: swap_rep(v, BIT_Y),
        lambda v: swap_shard(v, 1),
    )
    chosen = (bit_x, bit_y, bit_z)

    def loaded(other):
        layers = [2 * group + (1 - chosen[group] if other else chosen[group]) for group in range(GROUPS)]
        return load_layers(layers, activations, cotangents)

    gots = [swaps[group](value) for group, value in enumerate(loaded(True))]
    mine = loaded(False)
    sib = [swap_rep(value, CORE) for value in mine]
    fwds = [swap_rep(got, CORE) for got in gots]
    top = shard_count // 2
    low = (shard // top) & 1
    table = small_table(
        owners, [core, bit_x, bit_y, bit_z, chip, shard, place, low], shard, place, shard_count, slot_count
    )
    local = local_gradients(table, mine, sib, width, shard_count, half)
    (first, first_sent), (second, second_sent), (third, third_sent) = [
        layer_gradient(group, table, local[group], gots[group], fwds[group], width, shard_count, half)
        for group in range(GROUPS)
    ]

    def over_middle(values):
        bit = 2
        while bit < top:
            at = (shard // bit) & 1
            values = values.reshape(values.shape[0], -1, 2, half, columns)
            values = add(pick(values, at, 2), swap_shard(pick(values, 1 - at, 2), bit))
            bit *= 2
        bit = BIT_Y * 2
        while bit < replica_count:
            values = add(values, swap_rep(values, bit))
            bit *= 2
        return values

    first_got, second_got, third_got = (
        swaps[1](first_sent), swaps[2](second_sent), swap_shard(third_sent, top)
    )
    first = add(first, first_got).reshape(shard_count // 2, 2, half, columns)
    second = add(second, second_got)
    first_got = swaps[2](pick(first, 1 - bit_z, 1))
    second_got = swaps[0](pick(second, 1 - bit_x))
    third = add(third, third_got)
    third_got = swaps[0](pick(third, 1 - bit_x))
    first = add(pick(first, bit_z, 1), first_got)
    second = add(pick(second, bit_x), second_got)
    terms = jnp.stack([first, second]).reshape(2, 2, shard_count // 4, half, columns)
    terms = over_middle(terms.reshape(4, shard_count // 4, half, columns)).reshape(2, 2, half, columns)
    got = swap_shard(pick(terms, 1 - low, 1), top)
    third = add(pick(third, bit_x), third_got).reshape(shard_count // 4, 2, half, columns)
    third = over_middle(jnp.swapaxes(third, 0, 1)).reshape(2, half, columns)
    third_got = swaps[1](pick(third, 1 - bit_y))
    terms, last, sums = finish(
        1.0 / math.sqrt(token_total), table, terms, got, pick(third, bit_y), third_got
    )

    turned = [
        (r * shard_count + s, (r ^ BIT_Y) * shard_count + (s ^ 1))
        for r in range(replica_count)
        for s in range(shard_count)
        if ((r // BIT_Y) & 1) != (s & 1)
    ]
    moved = lax.ppermute(last, ("rep", "shard"), turned)
    last = jnp.where(bit_y == bit_z, last, moved)
    gradient = jnp.concatenate([terms, last[None]])

    for bit in (CORE, BIT_X, BIT_Y):
        sums = sums + swap_rep(sums, bit)
    bit = 1
    while bit < shard_count:
        sums = sums + swap_shard(sums, bit)
        bit *= 2
    factors = clip_factors(sums[0, :mats], bucket_starts, rows * width)

    old = jnp.stack(
        [
            lax.dynamic_slice(momentum, (matrix, core * half, 0), (1, half, columns)).reshape(half, columns)
            for matrix in (2 * bit_x + bit_y, CHIPS + chip, 2 * CHIPS + chip)
        ]
    )
    whole = newton_rows(table, factors, gradient, old, shard_count)
    whole = jnp.stack(
        [whole[0]]
        + [
            swap_shard(whole[k], k, lambda source, target: target < GROUPS)
            for k in range(1, shard_count)
        ]
    )
    whole_sib = swap_rep(whole, CORE)
    mixing = newton(table, whole, whole_sib)
    products = mixing[None]
    bit = 1
    while bit < shard_count:
        products = jnp.concatenate([products, swap_shard(products, bit)])
        bit *= 2
    products = jnp.stack([pick(products, shard ^ unit) for unit in range(GROUPS)])
    all_products = over_chips(products)
    all_products_sib = swap_rep(all_products, CORE)

    all_gradient = over_chips(gradient)
    all_gradient_sib = swap_rep(all_gradient, CORE)
    momentum_out, nesterov = momentum_step(table, factors, all_gradient, all_gradient_sib, momentum)

    carried = carried_rows(table, factors, all_gradient, momentum, shard_count)
    slot_rows = jnp.stack([swap_shard(carried[k - 1], k) for k in range(1, shard_count)])
    slot_rows = jnp.stack(
        [slot_rows] + [swap_rep(slot_rows, BIT_X * k) for k in range(1, slot_count)]
    )
    slot_rows_sib = swap_rep(slot_rows, CORE)

    update, owned = apply_step(
        update_scale, table, all_products, all_products_sib, nesterov, slot_rows, slot_rows_sib,
        shard_count,
    )
    return (momentum_out, update, owned)


def solution(mesh):
    placed = (
        P(None, ("rep", "shard"), None),
        P(None, ("rep", "shard"), None),
        P(None, None, "shard"),
        P(),
        P(),
    )
    return jax.shard_map(
        step,
        mesh=mesh,
        in_specs=placed,
        out_specs=(P(None, None, "shard"), P(None, None, "shard"), P("shard", None, None)),
        check_vma=False,
    )
```

```python
import functools
import math

import jax
import jax.numpy as jnp
from jax import lax
from jax.experimental import pallas as pl
from jax.experimental.pallas import tpu as pltpu
from jax.sharding import PartitionSpec as P

ITERS = 5

coef_a = 3.4445
coef_b = -4.775
coef_c = 2.0315
momentum_rate = 0.95
clip_level = 0.5
epsilon = 1e-06


F32 = jnp.float32
BF16 = jnp.bfloat16
NT = (((1,), (1,)), ((), ()))
NN = (((1,), (0,)), ((), ()))

CORE, BIT_X, BIT_Y = 1, 2, 4
CHIPS = 4
GROUPS = 3


def dot(a, b, dims):
    return lax.dot_general(a, b, dims, preferred_element_type=F32)


def swap_rep(value, bit):
    count = lax.axis_size("rep")
    return lax.ppermute(value, "rep", [(i, i ^ bit) for i in range(count)])


def swap_shard(value, bit, wanted=lambda source, target: True):
    count = lax.axis_size("shard")
    pairs = [(i, i ^ bit) for i in range(count) if wanted(i, i ^ bit)]
    return lax.ppermute(value, "shard", pairs)


def pick(value, index, axis=0):
    return lax.dynamic_index_in_dim(value, index, axis, keepdims=False)


def add(a, b):
    return (a.astype(F32) + b.astype(F32)).astype(BF16)


VMEM = pl.BlockSpec(memory_space=pltpu.VMEM)
ANY = pl.BlockSpec(memory_space=pl.ANY)
SMEM = pl.BlockSpec(memory_space=pltpu.SMEM)

AT_CORE, AT_X, AT_Y, AT_Z, AT_CHIP, AT_SHARD, AT_PLACE, AT_LOW, AT_LISTS = range(9)


def unit_of(matrix):
    return matrix // CHIPS


def chip_of(matrix):
    place = matrix % CHIPS
    turned = 2 * (place % 2) + place // 2
    if isinstance(matrix, int):
        return turned if matrix < CHIPS else place
    return jnp.where(matrix < CHIPS, turned, place)


def matrix_of(table, unit):
    chip = table[AT_CHIP]
    if isinstance(unit, int):
        return CHIPS * unit + chip if unit else 2 * table[AT_X] + table[AT_Y]
    return jnp.where(unit == 0, 2 * table[AT_X] + table[AT_Y], CHIPS * unit + chip)


def load_kernel(table, activations, cotangents, *rest):
    outs, sems = rest[:-1], rest[-1]
    width = activations.shape[2]
    copies = []
    for group, out in enumerate(outs):
        layer = table[group]
        copies.append(
            pltpu.make_async_copy(activations.at[layer], out.at[:, :width], sems.at[2 * group])
        )
        copies.append(
            pltpu.make_async_copy(cotangents.at[layer], out.at[:, width:], sems.at[2 * group + 1])
        )
    for copy in copies:
        copy.start()
    for copy in copies:
        copy.wait()


def load_layers(layers, activations, cotangents):
    _, tokens, width = activations.shape
    terms = cotangents.shape[2]
    return pl.pallas_call(
        load_kernel,
        in_specs=[SMEM, ANY, ANY],
        out_specs=[VMEM] * GROUPS,
        out_shape=[jax.ShapeDtypeStruct((tokens, width + terms), BF16)] * GROUPS,
        scratch_shapes=[pltpu.SemaphoreType.DMA((2 * GROUPS,))],
        cost_estimate=pl.CostEstimate(
            flops=GROUPS * tokens * width * 100, bytes_accessed=4 * GROUPS * tokens * (width + terms),
            transcendentals=0,
        ),
        name="load_layers",
    )(jnp.stack(layers), activations, cotangents)


def gradient_rows(table, group, width, half, sources, turned):
    for source, ref in enumerate(sources):
        tokens = ref.shape[0]
        for part in range(2):
            kind = part
            if group < GROUPS - 1:
                bit = table[AT_X if group else AT_Y]
                kind = 1 - bit if part else bit
            at = pl.multiple_of(width + (2 * kind + table[AT_CORE]) * half, half)
            turned[part * half:(part + 1) * half, source * tokens:(source + 1) * tokens] = ref[
                :, pl.ds(at, half)
            ].T


def local_kernel(width, blocks, table, mine0, mine1, mine2, sib0, sib1, sib2, out0, out1, out2, turned):
    half = turned.shape[1] // 2
    columns = width // blocks
    for group, (mine, sib, out) in enumerate(((mine0, sib0, out0), (mine1, sib1, out1), (mine2, sib2, out2))):
        sources = (mine, sib)
        gradient_rows(table, group, width, half, sources, turned.at[group])
        narrow = min(columns, 256)
        for start in range(0, width, narrow):
            span = slice(start, start + narrow)
            values = jnp.concatenate([ref[:, span] for ref in sources], axis=0)
            out[:, span] = dot(turned[group], values, NN)


def gradient_kernel(group, width, blocks, table, local, got, fwd, keep, send, turned):
    half = turned.shape[0] // 2
    columns = width // blocks
    sources = (got, fwd)
    gradient_rows(table, group, width, half, sources, turned)
    narrow = min(columns, 256)
    for start in range(0, width, narrow):
        span = slice(start, start + narrow)
        block, inner = start // columns, slice(start % columns, start % columns + narrow)
        values = jnp.concatenate([ref[:, span] for ref in sources], axis=0)
        terms = (local[:, span] + dot(turned[...], values, NN)).astype(BF16)
        if group < GROUPS - 1:
            keep[block, :, inner] = terms[:half]
            send[block, :, inner] = terms[half:]
            continue
        bit, value, at = table[AT_LOW], block // (blocks // 2), block % (blocks // 2)

        @pl.when(bit == value)
        def _():
            keep[0, at, :, inner] = terms[:half]
            keep[1, at, :, inner] = terms[half:]

        @pl.when(bit != value)
        def _():
            send[0, at, :, inner] = terms[:half]
            send[1, at, :, inner] = terms[half:]


def local_gradients(table, mine, sib, width, blocks, half):
    tokens = mine[0].shape[0]
    return pl.pallas_call(
        functools.partial(local_kernel, width, blocks),
        in_specs=[SMEM] + [VMEM] * 6,
        out_specs=[VMEM] * GROUPS,
        out_shape=[jax.ShapeDtypeStruct((2 * half, width), F32)] * GROUPS,
        scratch_shapes=[pltpu.VMEM((GROUPS, 2 * half, 2 * tokens), BF16)],
        cost_estimate=pl.CostEstimate(
            flops=GROUPS * 2 * 2 * tokens * 2 * half * width, bytes_accessed=GROUPS * 12 * tokens * width,
            transcendentals=0,
        ),
        name="local_gradients",
    )(table, *mine, *sib)


def layer_gradient(group, table, local, got, fwd, width, blocks, half):
    columns = width // blocks
    tokens = got.shape[0]
    shape = (blocks, half, columns) if group < GROUPS - 1 else (2, blocks // 2, half, columns)
    return pl.pallas_call(
        functools.partial(gradient_kernel, group, width, blocks),
        in_specs=[SMEM] + [VMEM] * 3,
        out_specs=[VMEM] * 2,
        out_shape=[jax.ShapeDtypeStruct(shape, BF16)] * 2,
        scratch_shapes=[pltpu.VMEM((2 * half, 2 * tokens), BF16)],
        cost_estimate=pl.CostEstimate(
            flops=2 * 2 * tokens * 2 * half * width, bytes_accessed=12 * tokens * width, transcendentals=0
        ),
        name="layer_gradient",
    )(table, local, got, fwd)


def finish_kernel(scale, table, keep0, got0, keep1, got1, keep2, got2, out, last, sums):
    lane = lax.broadcasted_iota(jnp.int32, sums.shape, 1)
    held = (
        matrix_of(table, 0),
        matrix_of(table, 1),
        2 * CHIPS + 2 * table[AT_Z] + table[AT_X],
    )
    total = jnp.zeros(sums.shape, F32)
    half = got0.shape[0]
    for unit, (keep, at, got) in enumerate(
        ((keep0, AT_LOW, got0), (keep1, AT_LOW, got1), (keep2, AT_Y, got2))
    ):
        partial = jnp.zeros((CHUNK, got.shape[1]), F32)
        for start in range(0, half, CHUNK):
            rows = slice(start, start + CHUNK)
            values = keep[table[at], rows, :].astype(F32) + got[rows, :].astype(F32)
            values = (values * scale).astype(BF16)
            if unit < GROUPS - 1:
                out[unit, rows, :] = values
            else:
                last[rows, :] = values
            wide = values.astype(F32)
            partial = partial + wide * wide
        total = total + jnp.where(lane == held[unit], jnp.sum(partial), 0.0)
    sums[...] = total


def finish(scale, table, *pairs):
    got = pairs[1]
    return pl.pallas_call(
        functools.partial(finish_kernel, scale),
        in_specs=[SMEM] + [VMEM] * 6,
        out_specs=[VMEM] * 3,
        out_shape=[
            jax.ShapeDtypeStruct((GROUPS - 1,) + got.shape, BF16),
            jax.ShapeDtypeStruct(got.shape, BF16),
            jax.ShapeDtypeStruct((1, 128), F32),
        ],
        cost_estimate=pl.CostEstimate(flops=1000 * got.size, bytes_accessed=8 * got.size, transcendentals=0),
        name="finish",
    )(table, *pairs)


CHUNK = 16


def momentum_kernel(table, factors, own, sib, momentum, momentum_out, nesterov):
    core, chip = table[AT_CORE], table[AT_CHIP]
    half = own.shape[2]
    for matrix in range(momentum.shape[0]):
        factor = factors[matrix]
        place, unit = chip_of(matrix) ^ chip, unit_of(matrix)
        for part, ref in ((core, own), (1 - core, sib)):

            def chunk(i, carry):
                source = pl.ds(pl.multiple_of(i * CHUNK, CHUNK), CHUNK)
                rows = pl.ds(pl.multiple_of(part * half + i * CHUNK, CHUNK), CHUNK)
                step = factor * ref[place, unit, source, :].astype(F32)
                fresh = momentum_rate * momentum[matrix, rows, :] + step
                momentum_out[matrix, rows, :] = fresh
                nesterov[matrix, rows, :] = (step + momentum_rate * fresh).astype(BF16)
                return carry

            lax.fori_loop(0, half // CHUNK, chunk, 0, unroll=2)


def momentum_step(table, factors, own, sib, momentum):
    mats, rows, columns = momentum.shape
    return pl.pallas_call(
        momentum_kernel,
        in_specs=[SMEM, SMEM, VMEM, VMEM, VMEM],
        out_specs=[VMEM, VMEM],
        out_shape=[
            jax.ShapeDtypeStruct(momentum.shape, F32),
            jax.ShapeDtypeStruct(momentum.shape, BF16),
        ],
        cost_estimate=pl.CostEstimate(
            flops=mats * rows * columns * 400, bytes_accessed=12 * mats * rows * columns, transcendentals=0
        ),
        name="momentum_step",
    )(table, factors, own, sib, momentum)


def input_rows(table, factor, gradient, momentum, matrix, out):
    half = out.shape[0]

    def chunk(i, carry):
        source = pl.ds(pl.multiple_of(i * CHUNK, CHUNK), CHUNK)
        rows = pl.ds(pl.multiple_of(table[AT_CORE] * half + i * CHUNK, CHUNK), CHUNK)
        step = factor * gradient(source).astype(F32)
        fresh = momentum_rate * momentum[matrix, rows, :] + step
        out[source, :] = (step + momentum_rate * fresh).astype(BF16)
        return carry

    lax.fori_loop(0, half // CHUNK, chunk, 0, unroll=2)


def rows_kernel(table, factors, gradient, momentum, *outs):
    for k, out in enumerate(outs):
        unit = jnp.minimum(table[AT_SHARD] ^ k, GROUPS - 1)
        matrix = matrix_of(table, unit)
        input_rows(
            table, factors[matrix], lambda rows, u=unit: gradient[u, rows, :], momentum, matrix, out
        )


def carried_kernel(table, factors, own, momentum, *outs):
    for k, out in enumerate(outs):
        matrix = table[AT_LISTS + (table[AT_SHARD] ^ (k + 1))]
        place, unit = chip_of(matrix) ^ table[AT_CHIP], unit_of(matrix)
        input_rows(
            table, factors[matrix], lambda rows, p=place, u=unit: own[p, u, rows, :], momentum, matrix, out
        )


def make_rows(kernel, count, table, factors, gradient, momentum):
    half, columns = gradient.shape[-2:]
    return pl.pallas_call(
        kernel,
        in_specs=[SMEM, SMEM, VMEM, VMEM],
        out_specs=[VMEM] * count,
        out_shape=[jax.ShapeDtypeStruct((half, columns), BF16)] * count,
        cost_estimate=pl.CostEstimate(
            flops=count * half * columns * 100, bytes_accessed=8 * count * half * columns, transcendentals=0
        ),
    )(table, factors, gradient, momentum)


def newton_kernel(table, own, sib, out, x, mix):
    core = table[AT_CORE]
    parts, half, columns = own.shape
    spans = [slice(p * columns, (p + 1) * columns) for p in range(parts)]
    total = jnp.zeros((1, 1), F32)
    for part, ref in ((core, own), (1 - core, sib)):
        rows = pl.ds(pl.multiple_of(part * half, half), half)
        for p, span in enumerate(spans):
            x[rows, span] = ref[p]
            wide = ref[p].astype(F32)
            total = total + jnp.sum(wide * wide)
    inverse = 1.0 / (jnp.sqrt(total) + epsilon)
    for span in spans:
        x[:, span] = (x[:, span].astype(F32) * inverse).astype(BF16)
    size = 2 * half
    diagonal = lax.broadcasted_iota(jnp.int32, (size, size), 0) == lax.broadcasted_iota(
        jnp.int32, (size, size), 1
    )
    for iteration in range(ITERS):
        gram = dot(x[...], x[...], NT).astype(BF16)
        square = dot(gram, gram, NN)
        mixing = (coef_b * gram.astype(F32) + coef_c * square).astype(BF16)
        if iteration < ITERS - 1:
            for span in spans:
                block = x[:, span]
                x[:, span] = (coef_a * block.astype(F32) + dot(mixing, block, NN)).astype(BF16)
        if iteration == 0:
            mix[...] = jnp.where(diagonal, coef_a, 0.0) + mixing.astype(F32)
        else:
            product = mix[...]
            high = product.astype(BF16)
            low = (product - high.astype(F32)).astype(BF16)
            mix[...] = coef_a * product + (dot(mixing, high, NN) + dot(mixing, low, NN))
    out[...] = (mix[pl.ds(pl.multiple_of(core * half, half), half), :] * inverse).astype(BF16)


def newton(table, own, sib):
    parts, half, columns = own.shape
    size = 2 * half
    return pl.pallas_call(
        newton_kernel,
        in_specs=[SMEM, VMEM, VMEM],
        out_specs=VMEM,
        scratch_shapes=[pltpu.VMEM((size, parts * columns), BF16), pltpu.VMEM((size, size), F32)],
        out_shape=jax.ShapeDtypeStruct((half, size), BF16),
        cost_estimate=pl.CostEstimate(
            flops=ITERS * 2 * size * size * (2 * parts * columns + 3 * size),
            bytes_accessed=8 * size * parts * columns, transcendentals=0,
        ),
        name="newton",
    )(table, own, sib)


def gather_rows(core, own, sib, out):
    half = own.shape[0]
    for part, block in ((core, own), (1 - core, sib)):
        out[pl.ds(pl.multiple_of(part * half, half), half), :] = block


def apply_kernel(scale, first, table, own, sib, values, own_rows, sib_rows, update, owned,
                 mix, rows, whole, held, sems):
    core, chip, shard = table[AT_CORE], table[AT_CHIP], table[AT_SHARD]
    mats = values.shape[0]
    slots, others, _, columns = own_rows.shape
    copies = []

    def leave(source, target):
        copies.append(pltpu.make_async_copy(source, target, sems.at[len(copies)]))
        copies[-1].start()

    for slot in range(slots):
        matrix = table[first + slot]
        filled = table[first + slots + slot] > 0
        place, unit = chip_of(matrix) ^ chip, unit_of(matrix)
        gather_rows(core, own[place, unit], sib[place, unit], mix.at[slot])
        at = table[AT_PLACE] ^ slot
        for k in range(others + 1):
            if k == 0:
                block = values[matrix]
            else:
                gather_rows(core, own_rows[at, k - 1], sib_rows[at, k - 1], rows.at[k - 1])
                block = rows[k - 1]
            result = scale * dot(mix[slot], block, NN).astype(BF16).astype(F32)
            span = pl.ds(pl.multiple_of((shard ^ k) * columns, columns), columns)
            held[slot, :, span] = jnp.where(filled, result, 0.0).astype(BF16)
        leave(held.at[slot], owned.at[slot])
    for matrix in range(mats):
        place, unit = chip_of(matrix) ^ chip, unit_of(matrix)
        gather_rows(core, own[place, unit], sib[place, unit], mix.at[slots + matrix])
        whole[matrix] = scale * dot(mix[slots + matrix], values[matrix], NN).astype(BF16).astype(F32)
        leave(whole.at[matrix], update.at[matrix])
    for copy in copies:
        copy.wait()


def apply_step(scale, table, own, sib, values, own_rows, sib_rows, shard_count):
    mats, rows, columns = values.shape
    slots, others, _, _ = own_rows.shape
    width = (others + 1) * columns
    return pl.pallas_call(
        functools.partial(apply_kernel, scale, AT_LISTS + shard_count),
        in_specs=[SMEM] + [VMEM] * 5,
        out_specs=[ANY, ANY],
        out_shape=[
            jax.ShapeDtypeStruct(values.shape, F32),
            jax.ShapeDtypeStruct((slots, rows, width), BF16),
        ],
        scratch_shapes=[
            pltpu.VMEM((slots + mats, rows, rows), BF16),
            pltpu.VMEM((others, rows, columns), BF16),
            pltpu.VMEM(values.shape, F32),
            pltpu.VMEM((slots, rows, width), BF16),
            pltpu.SemaphoreType.DMA((slots + mats,)),
        ],
        cost_estimate=pl.CostEstimate(
            flops=2 * rows * rows * (mats * columns + slots * width),
            bytes_accessed=6 * mats * rows * columns + 2 * slots * rows * width, transcendentals=0,
        ),
        name="apply_step",
    )(table, own, sib, values, own_rows, sib_rows)


def clip_factors(square_sums, bucket_starts, elements):
    mats = square_sums.shape[0]
    indices = jnp.arange(mats, dtype=jnp.int32)
    buckets = jnp.sum((indices[:, None] >= bucket_starts[None, :]).astype(jnp.int32), axis=1)
    together = (buckets[:, None] == buckets[None, :]).astype(F32)
    totals = jnp.sum(together * square_sums[None, :], axis=1)
    members = jnp.sum(together, axis=1)
    root_mean = jnp.sqrt(totals / (members * elements) + epsilon)
    return jnp.minimum(1.0, clip_level / root_mean)


def slot_numbers(owners):
    indices = jnp.arange(owners.shape[0], dtype=jnp.int32)
    earlier = (indices[None, :] < indices[:, None]) & (owners[None, :] == owners[:, None])
    return jnp.sum(earlier.astype(jnp.int32), axis=1)


def over_chips(value):
    return jnp.stack([value] + [swap_rep(value, BIT_X * k) for k in range(1, CHIPS)])


def small_table(owners, scalars, shard, place, shard_count, slot_count):
    indices = jnp.arange(owners.shape[0], dtype=jnp.int32)
    slot_of = slot_numbers(owners)
    holders = jnp.arange(shard_count, dtype=jnp.int32)
    places = jnp.arange(slot_count, dtype=jnp.int32)
    of_place = (holders[:, None] == owners[None, :]) & (slot_of == place)[None, :]
    of_shard = (places[:, None] == slot_of[None, :]) & (owners == shard)[None, :]
    return jnp.concatenate(
        [
            jnp.stack(scalars),
            jnp.sum(jnp.where(of_place, indices[None, :], 0), axis=1),
            jnp.sum(jnp.where(of_shard, indices[None, :], 0), axis=1),
            jnp.sum(of_shard.astype(jnp.int32), axis=1),
        ]
    )


def step(activations, cotangents, momentum, owners, bucket_starts):
    shard_count = lax.axis_size("shard")
    replica_count = lax.axis_size("rep")
    shard = lax.axis_index("shard")
    replica = lax.axis_index("rep")
    _, tokens, width = activations.shape
    mats, rows, columns = momentum.shape
    half = rows // 2
    token_total = tokens * shard_count * replica_count
    slot_count = -(-mats // shard_count) + 1
    update_scale = math.sqrt(max(rows, width))
    core = replica & 1
    bit_x = (replica >> 1) & 1
    bit_y = (replica >> 2) & 1
    bit_z = shard & 1
    chip = (replica >> 1) & (CHIPS - 1)
    place = chip % slot_count
    swaps = (
        lambda v: swap_rep(v, BIT_X),
        lambda v: swap_rep(v, BIT_Y),
        lambda v: swap_shard(v, 1),
    )
    chosen = (bit_x, bit_y, bit_z)

    def loaded(other):
        layers = [2 * group + (1 - chosen[group] if other else chosen[group]) for group in range(GROUPS)]
        return load_layers(layers, activations, cotangents)

    gots = []
    for group, value in enumerate(loaded(True)):
        gots.append(swaps[group](value))
    mine = loaded(False)
    sib = [swap_rep(value, CORE) for value in mine]
    fwds = []
    for got in gots:
        fwds.append(swap_rep(got, CORE))
    top = shard_count // 2
    low = (shard // top) & 1
    table = small_table(
        owners, [core, bit_x, bit_y, bit_z, chip, shard, place, low], shard, place, shard_count, slot_count
    )
    local = local_gradients(table, mine, sib, width, shard_count, half)
    gradients = []
    for group in range(GROUPS):
        gradients.append(layer_gradient(group, table, local[group], gots[group], fwds[group], width, shard_count, half))
    (first, first_sent), (second, second_sent), (third, third_sent) = gradients

    def over_middle(values):
        bit = 2
        while bit < top:
            at = (shard // bit) & 1
            values = values.reshape(values.shape[0], -1, 2, half, columns)
            values = add(pick(values, at, 2), swap_shard(pick(values, 1 - at, 2), bit))
            bit *= 2
        bit = BIT_Y * 2
        while bit < replica_count:
            values = add(values, swap_rep(values, bit))
            bit *= 2
        return values

    first_got = swaps[1](first_sent)
    second_got = swaps[0](second_sent)
    third_got = swap_shard(third_sent, top)
    first = add(first, first_got).reshape(shard_count // 2, 2, half, columns)
    first_got = swaps[2](pick(first, 1 - bit_z, 1))
    second = add(second, second_got).reshape(shard_count // 2, 2, half, columns)
    second_got = swaps[2](pick(second, 1 - bit_z, 1))
    third = add(third, third_got)
    third_got = swaps[0](pick(third, 1 - bit_x))
    pairs = []
    for value, got in ((first, first_got), (second, second_got)):
        value = add(pick(value, bit_z, 1), got).reshape(2, shard_count // 4, half, columns)
        value = over_middle(value).reshape(2, half, columns)
        pairs += [value, swap_shard(pick(value, 1 - low), top)]
    third = add(pick(third, bit_x), third_got).reshape(shard_count // 4, 2, half, columns)
    third = over_middle(jnp.swapaxes(third, 0, 1)).reshape(2, half, columns)
    pairs += [third, swaps[1](pick(third, 1 - bit_y))]
    terms, last, sums = finish(1.0 / math.sqrt(token_total), table, *pairs)

    turned = [
        (r * shard_count + s, (r ^ BIT_Y) * shard_count + (s ^ 1))
        for r in range(replica_count)
        for s in range(shard_count)
        if ((r // BIT_Y) & 1) != (s & 1)
    ]
    moved = lax.ppermute(last, ("rep", "shard"), turned)
    last = jnp.where(bit_y == bit_z, last, moved)
    gradient = jnp.concatenate([terms, last[None]])

    for bit in (CORE, BIT_X, BIT_Y):
        sums = sums + swap_rep(sums, bit)
    bit = 1
    while bit < shard_count:
        sums = sums + swap_shard(sums, bit)
        bit *= 2
    factors = clip_factors(sums[0, :mats], bucket_starts, rows * width)

    whole = make_rows(rows_kernel, shard_count, table, factors, gradient, momentum)
    whole = jnp.stack(
        [whole[0]]
        + [
            swap_shard(whole[k], k, lambda source, target: target < GROUPS)
            for k in range(1, shard_count)
        ]
    )
    whole_sib = swap_rep(whole, CORE)
    mixing = newton(table, whole, whole_sib)
    products = mixing[None]
    bit = 1
    while bit < shard_count:
        products = jnp.concatenate([products, swap_shard(products, bit)])
        bit *= 2
    products = jnp.stack([pick(products, shard ^ unit) for unit in range(GROUPS)])
    all_products = over_chips(products)
    all_products_sib = swap_rep(all_products, CORE)

    all_gradient = over_chips(gradient)
    all_gradient_sib = swap_rep(all_gradient, CORE)
    momentum_out, nesterov = momentum_step(table, factors, all_gradient, all_gradient_sib, momentum)

    carried = make_rows(carried_kernel, shard_count - 1, table, factors, all_gradient, momentum)
    slot_rows = jnp.stack([swap_shard(carried[k - 1], k) for k in range(1, shard_count)])
    slot_rows = jnp.stack(
        [slot_rows] + [swap_rep(slot_rows, BIT_X * k) for k in range(1, slot_count)]
    )
    slot_rows_sib = swap_rep(slot_rows, CORE)

    update, owned = apply_step(
        update_scale, table, all_products, all_products_sib, nesterov, slot_rows, slot_rows_sib,
        shard_count,
    )
    return (momentum_out, update, owned)


def solution(mesh):
    placed = (
        P(None, ("rep", "shard"), None),
        P(None, ("rep", "shard"), None),
        P(None, None, "shard"),
        P(),
        P(),
    )
    return jax.shard_map(
        step,
        mesh=mesh,
        in_specs=placed,
        out_specs=(P(None, None, "shard"), P(None, None, "shard"), P("shard", None, None)),
        check_vma=False,
    )
```

```python
import functools
import math

import jax
import jax.numpy as jnp
from jax import lax
from jax.experimental import pallas as pl
from jax.experimental.pallas import tpu as pltpu
from jax.sharding import PartitionSpec as P

ITERS = 5

coef_a = 3.4445
coef_b = -4.775
coef_c = 2.0315
momentum_rate = 0.95
clip_level = 0.5
epsilon = 1e-06


F32 = jnp.float32
BF16 = jnp.bfloat16
NT = (((1,), (1,)), ((), ()))
NN = (((1,), (0,)), ((), ()))

CORE, BIT_X, BIT_Y = 1, 2, 4
CHIPS = 4
GROUPS = 3


def dot(a, b, dims):
    return lax.dot_general(a, b, dims, preferred_element_type=F32)


def swap_rep(value, bit):
    count = lax.axis_size("rep")
    return lax.ppermute(value, "rep", [(i, i ^ bit) for i in range(count)])


def swap_shard(value, bit, wanted=lambda source, target: True):
    count = lax.axis_size("shard")
    pairs = [(i, i ^ bit) for i in range(count) if wanted(i, i ^ bit)]
    return lax.ppermute(value, "shard", pairs)


def pick(value, index, axis=0):
    return lax.dynamic_index_in_dim(value, index, axis, keepdims=False)


def add(a, b):
    return (a.astype(F32) + b.astype(F32)).astype(BF16)


VMEM = pl.BlockSpec(memory_space=pltpu.VMEM)
HBM = pl.BlockSpec(memory_space=pltpu.HBM)
SMEM = pl.BlockSpec(memory_space=pltpu.SMEM)
CHUNK = 16
SMALL = pltpu.CompilerParams(vmem_limit_bytes=16 << 20)
LARGE = pltpu.CompilerParams(vmem_limit_bytes=32 << 20)

AT_CORE, AT_X, AT_Y, AT_Z, AT_CHIP, AT_SHARD, AT_PLACE, AT_LOW, AT_LISTS = range(9)


def unit_of(matrix):
    return matrix // CHIPS


def chip_of(matrix):
    place = matrix % CHIPS
    turned = 2 * (place % 2) + place // 2
    if isinstance(matrix, int):
        return turned if matrix < CHIPS else place
    return jnp.where(matrix < CHIPS, turned, place)


def matrix_of(table, unit):
    chip = table[AT_CHIP]
    if isinstance(unit, int):
        return CHIPS * unit + chip if unit else 2 * table[AT_X] + table[AT_Y]
    return jnp.where(unit == 0, 2 * table[AT_X] + table[AT_Y], CHIPS * unit + chip)


def load_kernel(table, activations, cotangents, *rest):
    outs, sems = rest[:-1], rest[-1]
    width = activations.shape[2]
    copies = []
    for group, out in enumerate(outs):
        layer = table[group]
        copies.append(
            pltpu.make_async_copy(activations.at[layer], out.at[:, :width], sems.at[2 * group])
        )
        copies.append(
            pltpu.make_async_copy(cotangents.at[layer], out.at[:, width:], sems.at[2 * group + 1])
        )
    for copy in copies:
        copy.start()
    for copy in copies:
        copy.wait()


def load_layers(layers, activations, cotangents):
    _, tokens, width = activations.shape
    terms = cotangents.shape[2]
    return pl.pallas_call(
        load_kernel,
        in_specs=[SMEM, HBM, HBM],
        out_specs=[VMEM] * GROUPS,
        out_shape=[jax.ShapeDtypeStruct((tokens, width + terms), BF16)] * GROUPS,
        scratch_shapes=[pltpu.SemaphoreType.DMA((2 * GROUPS,))],
        cost_estimate=pl.CostEstimate(
            flops=GROUPS * tokens * width * 100, bytes_accessed=4 * GROUPS * tokens * (width + terms),
            transcendentals=0,
        ),
        compiler_params=SMALL,
        name="load_layers",
    )(jnp.stack(layers), activations, cotangents)


def gradient_rows(table, group, width, half, sources, turned):
    for source, ref in enumerate(sources):
        tokens = ref.shape[0]
        for part in range(2):
            kind = part
            if group < GROUPS - 1:
                bit = table[AT_X if group else AT_Y]
                kind = 1 - bit if part else bit
            at = pl.multiple_of(width + (2 * kind + table[AT_CORE]) * half, half)
            turned[part * half:(part + 1) * half, source * tokens:(source + 1) * tokens] = ref[
                :, pl.ds(at, half)
            ].T


def local_kernel(width, blocks, table, mine0, mine1, mine2, sib0, sib1, sib2, out0, out1, out2, turned):
    half = turned.shape[1] // 2
    columns = width // blocks
    for group, (mine, sib, out) in enumerate(((mine0, sib0, out0), (mine1, sib1, out1), (mine2, sib2, out2))):
        sources = (mine, sib)
        gradient_rows(table, group, width, half, sources, turned.at[group])
        narrow = min(columns, 256)
        for start in range(0, width, narrow):
            span = slice(start, start + narrow)
            values = jnp.concatenate([ref[:, span] for ref in sources], axis=0)
            out[:, span] = dot(turned[group], values, NN)


def gradient_kernel(group, width, blocks, table, local, got, fwd, keep, send, turned):
    half = turned.shape[0] // 2
    columns = width // blocks
    sources = (got, fwd)
    gradient_rows(table, group, width, half, sources, turned)
    narrow = min(columns, 256)
    for start in range(0, width, narrow):
        span = slice(start, start + narrow)
        block, inner = start // columns, slice(start % columns, start % columns + narrow)
        values = jnp.concatenate([ref[:, span] for ref in sources], axis=0)
        terms = (local[:, span] + dot(turned[...], values, NN)).astype(BF16)
        if group < GROUPS - 1:
            keep[block, :, inner] = terms[:half]
            send[block, :, inner] = terms[half:]
            continue
        bit, value, at = table[AT_LOW], block // (blocks // 2), block % (blocks // 2)

        @pl.when(bit == value)
        def _():
            keep[0, at, :, inner] = terms[:half]
            keep[1, at, :, inner] = terms[half:]

        @pl.when(bit != value)
        def _():
            send[0, at, :, inner] = terms[:half]
            send[1, at, :, inner] = terms[half:]


def local_gradients(table, mine, sib, width, blocks, half):
    tokens = mine[0].shape[0]
    return pl.pallas_call(
        functools.partial(local_kernel, width, blocks),
        in_specs=[SMEM] + [VMEM] * 6,
        out_specs=[VMEM] * GROUPS,
        out_shape=[jax.ShapeDtypeStruct((2 * half, width), F32)] * GROUPS,
        scratch_shapes=[pltpu.VMEM((GROUPS, 2 * half, 2 * tokens), BF16)],
        cost_estimate=pl.CostEstimate(
            flops=GROUPS * 2 * 2 * tokens * 2 * half * width, bytes_accessed=GROUPS * 12 * tokens * width,
            transcendentals=0,
        ),
        compiler_params=LARGE,
        name="local_gradients",
    )(table, *mine, *sib)


def layer_gradient(group, table, local, got, fwd, width, blocks, half):
    columns = width // blocks
    tokens = got.shape[0]
    shape = (blocks, half, columns) if group < GROUPS - 1 else (2, blocks // 2, half, columns)
    return pl.pallas_call(
        functools.partial(gradient_kernel, group, width, blocks),
        in_specs=[SMEM] + [VMEM] * 3,
        out_specs=[VMEM] * 2,
        out_shape=[jax.ShapeDtypeStruct(shape, BF16)] * 2,
        scratch_shapes=[pltpu.VMEM((2 * half, 2 * tokens), BF16)],
        cost_estimate=pl.CostEstimate(
            flops=2 * 2 * tokens * 2 * half * width, bytes_accessed=12 * tokens * width, transcendentals=0
        ),
        compiler_params=SMALL,
        name="layer_gradient",
    )(table, local, got, fwd)


def finish_kernel(scale, table, keep0, got0, keep1, got1, keep2, got2, out, last, sums):
    lane = lax.broadcasted_iota(jnp.int32, sums.shape, 1)
    held = (
        matrix_of(table, 0),
        matrix_of(table, 1),
        2 * CHIPS + 2 * table[AT_Z] + table[AT_X],
    )
    total = jnp.zeros(sums.shape, F32)
    half = got0.shape[0]
    for unit, (keep, at, got) in enumerate(
        ((keep0, AT_LOW, got0), (keep1, AT_LOW, got1), (keep2, AT_Y, got2))
    ):
        partial = jnp.zeros((CHUNK, got.shape[1]), F32)
        for start in range(0, half, CHUNK):
            rows = slice(start, start + CHUNK)
            values = keep[table[at], rows, :].astype(F32) + got[rows, :].astype(F32)
            values = (values * scale).astype(BF16)
            if unit < GROUPS - 1:
                out[unit, rows, :] = values
            else:
                last[rows, :] = values
            wide = values.astype(F32)
            partial = partial + wide * wide
        total = total + jnp.where(lane == held[unit], jnp.sum(partial), 0.0)
    sums[...] = total


def finish(scale, table, *pairs):
    got = pairs[1]
    return pl.pallas_call(
        functools.partial(finish_kernel, scale),
        in_specs=[SMEM] + [VMEM] * 6,
        out_specs=[VMEM] * 3,
        out_shape=[
            jax.ShapeDtypeStruct((GROUPS - 1,) + got.shape, BF16),
            jax.ShapeDtypeStruct(got.shape, BF16),
            jax.ShapeDtypeStruct((1, 128), F32),
        ],
        cost_estimate=pl.CostEstimate(flops=1000 * got.size, bytes_accessed=8 * got.size, transcendentals=0),
        compiler_params=SMALL,
        name="finish",
    )(table, *pairs)


def momentum_kernel(table, factors, own, sib, momentum, momentum_out, nesterov, buffer, inputs, came, left, gone):
    core, chip = table[AT_CORE], table[AT_CHIP]
    half = own.shape[2]
    mats = buffer.shape[0]
    ins = [pltpu.make_async_copy(momentum.at[m], buffer.at[m], came.at[m]) for m in range(mats)]
    outs = [pltpu.make_async_copy(buffer.at[m], momentum_out.at[m], left.at[m]) for m in range(mats)]
    outs += [pltpu.make_async_copy(inputs.at[m], nesterov.at[m], gone.at[m]) for m in range(mats)]
    for copy in ins:
        copy.start()
    for matrix in range(mats):
        ins[matrix].wait()
        factor = factors[matrix]
        place, unit = chip_of(matrix) ^ chip, unit_of(matrix)
        for part, ref in ((core, own), (1 - core, sib)):

            def chunk(i, carry):
                source = pl.ds(pl.multiple_of(i * CHUNK, CHUNK), CHUNK)
                rows = pl.ds(pl.multiple_of(part * half + i * CHUNK, CHUNK), CHUNK)
                step = factor * ref[place, unit, source, :].astype(F32)
                fresh = momentum_rate * buffer[matrix, rows, :] + step
                buffer[matrix, rows, :] = fresh
                inputs[matrix, rows, :] = (step + momentum_rate * fresh).astype(BF16)
                return carry

            lax.fori_loop(0, half // CHUNK, chunk, 0, unroll=4)
        outs[matrix].start()
        outs[mats + matrix].start()
    for copy in outs:
        copy.wait()


def momentum_step(table, factors, own, sib, momentum):
    mats, rows, columns = momentum.shape
    return pl.pallas_call(
        momentum_kernel,
        in_specs=[SMEM, SMEM, VMEM, VMEM, HBM],
        out_specs=[HBM, HBM],
        out_shape=[
            jax.ShapeDtypeStruct(momentum.shape, F32),
            jax.ShapeDtypeStruct(momentum.shape, BF16),
        ],
        scratch_shapes=[
            pltpu.VMEM(momentum.shape, F32),
            pltpu.VMEM(momentum.shape, BF16),
            pltpu.SemaphoreType.DMA((mats,)),
            pltpu.SemaphoreType.DMA((mats,)),
            pltpu.SemaphoreType.DMA((mats,)),
        ],
        compiler_params=LARGE,
        cost_estimate=pl.CostEstimate(
            flops=mats * rows * columns * 400, bytes_accessed=12 * mats * rows * columns, transcendentals=0
        ),
        name="momentum_step",
    )(table, factors, own, sib, momentum)


def input_rows(table, factors, gradients, matrices, momentum, outs, buffer, sems):
    half = outs[0].shape[0]
    part = pl.ds(pl.multiple_of(table[AT_CORE] * half, half), half)
    copies = [
        pltpu.make_async_copy(momentum.at[matrix, part, :], buffer.at[k], sems.at[k])
        for k, matrix in enumerate(matrices)
    ]
    for copy in copies:
        copy.start()
    for k, (gradient, matrix, out) in enumerate(zip(gradients, matrices, outs)):
        copies[k].wait()
        factor = factors[matrix]

        def chunk(i, carry):
            rows = pl.ds(pl.multiple_of(i * CHUNK, CHUNK), CHUNK)
            step = factor * gradient(rows).astype(F32)
            fresh = momentum_rate * buffer[k, rows, :] + step
            out[rows, :] = (step + momentum_rate * fresh).astype(BF16)
            return carry

        lax.fori_loop(0, half // CHUNK, chunk, 0, unroll=4)


def rows_kernel(table, factors, gradient, momentum, *rest):
    outs, (buffer, sems) = rest[:-2], rest[-2:]
    units = [jnp.minimum(table[AT_SHARD] ^ k, GROUPS - 1) for k in range(len(outs))]
    gradients = [lambda rows, u=unit: gradient[u, rows, :] for unit in units]
    input_rows(
        table, factors, gradients, [matrix_of(table, unit) for unit in units], momentum, outs, buffer, sems
    )


def carried_kernel(table, factors, own, momentum, *rest):
    outs, (buffer, sems) = rest[:-2], rest[-2:]
    matrices = [table[AT_LISTS + (table[AT_SHARD] ^ (k + 1))] for k in range(len(outs))]
    gradients = [
        lambda rows, p=chip_of(matrix) ^ table[AT_CHIP], u=unit_of(matrix): own[p, u, rows, :]
        for matrix in matrices
    ]
    input_rows(table, factors, gradients, matrices, momentum, outs, buffer, sems)


def make_rows(kernel, count, table, factors, gradient, momentum):
    half, columns = gradient.shape[-2:]
    return pl.pallas_call(
        kernel,
        in_specs=[SMEM, SMEM, VMEM, HBM],
        out_specs=[VMEM] * count,
        out_shape=[jax.ShapeDtypeStruct((half, columns), BF16)] * count,
        scratch_shapes=[pltpu.VMEM((count, half, columns), F32), pltpu.SemaphoreType.DMA((count,))],
        compiler_params=SMALL,
        cost_estimate=pl.CostEstimate(
            flops=count * half * columns * 100, bytes_accessed=8 * count * half * columns, transcendentals=0
        ),
    )(table, factors, gradient, momentum)


def newton_kernel(table, own, sib, out, x, mix):
    core = table[AT_CORE]
    parts, half, columns = own.shape
    spans = [slice(p * columns, (p + 1) * columns) for p in range(parts)]
    total = jnp.zeros((1, 1), F32)
    for part, ref in ((core, own), (1 - core, sib)):
        rows = pl.ds(pl.multiple_of(part * half, half), half)
        for p, span in enumerate(spans):
            x[rows, span] = ref[p]
            wide = ref[p].astype(F32)
            total = total + jnp.sum(wide * wide)
    inverse = 1.0 / (jnp.sqrt(total) + epsilon)
    for span in spans:
        x[:, span] = (x[:, span].astype(F32) * inverse).astype(BF16)
    size = 2 * half
    diagonal = lax.broadcasted_iota(jnp.int32, (size, size), 0) == lax.broadcasted_iota(
        jnp.int32, (size, size), 1
    )
    for iteration in range(ITERS):
        gram = dot(x[...], x[...], NT).astype(BF16)
        square = dot(gram, gram, NN)
        mixing = (coef_b * gram.astype(F32) + coef_c * square).astype(BF16)
        if iteration < ITERS - 1:
            for span in spans:
                block = x[:, span]
                x[:, span] = (coef_a * block.astype(F32) + dot(mixing, block, NN)).astype(BF16)
        if iteration == 0:
            mix[...] = jnp.where(diagonal, coef_a, 0.0) + mixing.astype(F32)
        else:
            product = mix[...]
            high = product.astype(BF16)
            low = (product - high.astype(F32)).astype(BF16)
            mix[...] = coef_a * product + (dot(mixing, high, NN) + dot(mixing, low, NN))
    out[...] = (mix[pl.ds(pl.multiple_of(core * half, half), half), :] * inverse).astype(BF16)


def newton(table, own, sib):
    parts, half, columns = own.shape
    size = 2 * half
    return pl.pallas_call(
        newton_kernel,
        in_specs=[SMEM, VMEM, VMEM],
        out_specs=VMEM,
        scratch_shapes=[pltpu.VMEM((size, parts * columns), BF16), pltpu.VMEM((size, size), F32)],
        out_shape=jax.ShapeDtypeStruct((half, size), BF16),
        cost_estimate=pl.CostEstimate(
            flops=ITERS * 2 * size * size * (2 * parts * columns + 3 * size),
            bytes_accessed=8 * size * parts * columns, transcendentals=0,
        ),
        compiler_params=SMALL,
        name="newton",
    )(table, own, sib)


def gather_rows(core, own, sib, out):
    half = own.shape[0]
    for part, block in ((core, own), (1 - core, sib)):
        out[pl.ds(pl.multiple_of(part * half, half), half), :] = block


def apply_kernel(scale, first, table, own, sib, values, own_rows, sib_rows, update, owned,
                 mix, rows, whole, held, sems):
    core, chip, shard = table[AT_CORE], table[AT_CHIP], table[AT_SHARD]
    mats = values.shape[0]
    slots, others, _, columns = own_rows.shape
    copies = []

    def leave(source, target):
        copies.append(pltpu.make_async_copy(source, target, sems.at[len(copies)]))
        copies[-1].start()

    for slot in range(slots):
        matrix = table[first + slot]
        filled = table[first + slots + slot] > 0
        place, unit = chip_of(matrix) ^ chip, unit_of(matrix)
        gather_rows(core, own[place, unit], sib[place, unit], mix.at[slot])
        at = table[AT_PLACE] ^ slot
        for k in range(others + 1):
            if k == 0:
                block = values[matrix]
            else:
                gather_rows(core, own_rows[at, k - 1], sib_rows[at, k - 1], rows.at[k - 1])
                block = rows[k - 1]
            result = scale * dot(mix[slot], block, NN).astype(BF16).astype(F32)
            span = pl.ds(pl.multiple_of((shard ^ k) * columns, columns), columns)
            held[slot, :, span] = jnp.where(filled, result, 0.0).astype(BF16)
        leave(held.at[slot], owned.at[slot])
    for matrix in range(mats):
        place, unit = chip_of(matrix) ^ chip, unit_of(matrix)
        gather_rows(core, own[place, unit], sib[place, unit], mix.at[slots + matrix])
        whole[matrix] = scale * dot(mix[slots + matrix], values[matrix], NN).astype(BF16).astype(F32)
        leave(whole.at[matrix], update.at[matrix])
    for copy in copies:
        copy.wait()


def apply_step(scale, table, own, sib, values, own_rows, sib_rows, shard_count):
    mats, rows, columns = values.shape
    slots, others, _, _ = own_rows.shape
    width = (others + 1) * columns
    return pl.pallas_call(
        functools.partial(apply_kernel, scale, AT_LISTS + shard_count),
        in_specs=[SMEM] + [VMEM] * 5,
        out_specs=[HBM, HBM],
        out_shape=[
            jax.ShapeDtypeStruct(values.shape, F32),
            jax.ShapeDtypeStruct((slots, rows, width), BF16),
        ],
        scratch_shapes=[
            pltpu.VMEM((slots + mats, rows, rows), BF16),
            pltpu.VMEM((others, rows, columns), BF16),
            pltpu.VMEM(values.shape, F32),
            pltpu.VMEM((slots, rows, width), BF16),
            pltpu.SemaphoreType.DMA((slots + mats,)),
        ],
        cost_estimate=pl.CostEstimate(
            flops=2 * rows * rows * (mats * columns + slots * width),
            bytes_accessed=6 * mats * rows * columns + 2 * slots * rows * width, transcendentals=0,
        ),
        compiler_params=LARGE,
        name="apply_step",
    )(table, own, sib, values, own_rows, sib_rows)


def clip_factors(square_sums, bucket_starts, elements):
    mats = square_sums.shape[0]
    indices = jnp.arange(mats, dtype=jnp.int32)
    buckets = jnp.sum((indices[:, None] >= bucket_starts[None, :]).astype(jnp.int32), axis=1)
    together = (buckets[:, None] == buckets[None, :]).astype(F32)
    totals = jnp.sum(together * square_sums[None, :], axis=1)
    members = jnp.sum(together, axis=1)
    root_mean = jnp.sqrt(totals / (members * elements) + epsilon)
    return jnp.minimum(1.0, clip_level / root_mean)


def slot_numbers(owners):
    indices = jnp.arange(owners.shape[0], dtype=jnp.int32)
    earlier = (indices[None, :] < indices[:, None]) & (owners[None, :] == owners[:, None])
    return jnp.sum(earlier.astype(jnp.int32), axis=1)


def over_chips(value):
    return jnp.stack([value] + [swap_rep(value, BIT_X * k) for k in range(1, CHIPS)])


def small_table(owners, scalars, shard, place, shard_count, slot_count):
    indices = jnp.arange(owners.shape[0], dtype=jnp.int32)
    slot_of = slot_numbers(owners)
    holders = jnp.arange(shard_count, dtype=jnp.int32)
    places = jnp.arange(slot_count, dtype=jnp.int32)
    of_place = (holders[:, None] == owners[None, :]) & (slot_of == place)[None, :]
    of_shard = (places[:, None] == slot_of[None, :]) & (owners == shard)[None, :]
    return jnp.concatenate(
        [
            jnp.stack(scalars),
            jnp.sum(jnp.where(of_place, indices[None, :], 0), axis=1),
            jnp.sum(jnp.where(of_shard, indices[None, :], 0), axis=1),
            jnp.sum(of_shard.astype(jnp.int32), axis=1),
        ]
    )


def step(activations, cotangents, momentum, owners, bucket_starts):
    shard_count = lax.axis_size("shard")
    replica_count = lax.axis_size("rep")
    shard = lax.axis_index("shard")
    replica = lax.axis_index("rep")
    _, tokens, width = activations.shape
    mats, rows, columns = momentum.shape
    half = rows // 2
    token_total = tokens * shard_count * replica_count
    slot_count = -(-mats // shard_count) + 1
    update_scale = math.sqrt(max(rows, width))
    core = replica & 1
    bit_x = (replica >> 1) & 1
    bit_y = (replica >> 2) & 1
    bit_z = shard & 1
    chip = (replica >> 1) & (CHIPS - 1)
    place = chip % slot_count
    swaps = (
        lambda v: swap_rep(v, BIT_X),
        lambda v: swap_rep(v, BIT_Y),
        lambda v: swap_shard(v, 1),
    )
    chosen = (bit_x, bit_y, bit_z)

    def loaded(other):
        layers = [2 * group + (1 - chosen[group] if other else chosen[group]) for group in range(GROUPS)]
        return load_layers(layers, activations, cotangents)

    gots = []
    for group, value in enumerate(loaded(True)):
        gots.append(swaps[group](value))
    mine = loaded(False)
    sib = [swap_rep(value, CORE) for value in mine]
    fwds = []
    for got in gots:
        fwds.append(swap_rep(got, CORE))
    top = shard_count // 2
    low = (shard // top) & 1
    table = small_table(
        owners, [core, bit_x, bit_y, bit_z, chip, shard, place, low], shard, place, shard_count, slot_count
    )
    local = local_gradients(table, mine, sib, width, shard_count, half)
    gradients = []
    for group in range(GROUPS):
        gradients.append(layer_gradient(group, table, local[group], gots[group], fwds[group], width, shard_count, half))
    (first, first_sent), (second, second_sent), (third, third_sent) = gradients

    def over_middle(values):
        bit = 2
        while bit < top:
            at = (shard // bit) & 1
            values = values.reshape(values.shape[0], -1, 2, half, columns)
            values = add(pick(values, at, 2), swap_shard(pick(values, 1 - at, 2), bit))
            bit *= 2
        bit = BIT_Y * 2
        while bit < replica_count:
            values = add(values, swap_rep(values, bit))
            bit *= 2
        return values

    first_got = swaps[1](first_sent)
    second_got = swaps[0](second_sent)
    third_got = swap_shard(third_sent, top)
    first = add(first, first_got).reshape(shard_count // 2, 2, half, columns)
    first_got = swaps[2](pick(first, 1 - bit_z, 1))
    second = add(second, second_got).reshape(shard_count // 2, 2, half, columns)
    second_got = swaps[2](pick(second, 1 - bit_z, 1))
    third = add(third, third_got)
    third_got = swaps[0](pick(third, 1 - bit_x))
    pairs = []
    for value, got in ((first, first_got), (second, second_got)):
        value = add(pick(value, bit_z, 1), got).reshape(2, shard_count // 4, half, columns)
        value = over_middle(value).reshape(2, half, columns)
        pairs += [value, swap_shard(pick(value, 1 - low), top)]
    third = add(pick(third, bit_x), third_got).reshape(shard_count // 4, 2, half, columns)
    third = over_middle(jnp.swapaxes(third, 0, 1)).reshape(2, half, columns)
    pairs += [third, swaps[1](pick(third, 1 - bit_y))]
    terms, last, sums = finish(1.0 / math.sqrt(token_total), table, *pairs)

    turned = [
        (r * shard_count + s, (r ^ BIT_Y) * shard_count + (s ^ 1))
        for r in range(replica_count)
        for s in range(shard_count)
        if ((r // BIT_Y) & 1) != (s & 1)
    ]
    moved = lax.ppermute(last, ("rep", "shard"), turned)
    last = jnp.where(bit_y == bit_z, last, moved)
    gradient = jnp.concatenate([terms, last[None]])

    for bit in (CORE, BIT_X, BIT_Y):
        sums = sums + swap_rep(sums, bit)
    bit = 1
    while bit < shard_count:
        sums = sums + swap_shard(sums, bit)
        bit *= 2
    factors = clip_factors(sums[0, :mats], bucket_starts, rows * width)

    whole = make_rows(rows_kernel, shard_count, table, factors, gradient, momentum)
    whole = jnp.stack(
        [whole[0]]
        + [
            swap_shard(whole[k], k, lambda source, target: target < GROUPS)
            for k in range(1, shard_count)
        ]
    )
    whole_sib = swap_rep(whole, CORE)
    mixing = newton(table, whole, whole_sib)
    products = mixing[None]
    bit = 1
    while bit < shard_count:
        products = jnp.concatenate([products, swap_shard(products, bit)])
        bit *= 2
    products = jnp.stack([pick(products, shard ^ unit) for unit in range(GROUPS)])
    all_products = over_chips(products)
    all_products_sib = swap_rep(all_products, CORE)

    all_gradient = over_chips(gradient)
    all_gradient_sib = swap_rep(all_gradient, CORE)
    momentum_out, nesterov = momentum_step(table, factors, all_gradient, all_gradient_sib, momentum)

    carried = make_rows(carried_kernel, shard_count - 1, table, factors, all_gradient, momentum)
    slot_rows = jnp.stack([swap_shard(carried[k - 1], k) for k in range(1, shard_count)])
    slot_rows = jnp.stack(
        [slot_rows] + [swap_rep(slot_rows, BIT_X * k) for k in range(1, slot_count)]
    )
    slot_rows_sib = swap_rep(slot_rows, CORE)

    update, owned = apply_step(
        update_scale, table, all_products, all_products_sib, nesterov, slot_rows, slot_rows_sib,
        shard_count,
    )
    return (momentum_out, update, owned)


def solution(mesh):
    placed = (
        P(None, ("rep", "shard"), None),
        P(None, ("rep", "shard"), None),
        P(None, None, "shard"),
        P(),
        P(),
    )
    return jax.shard_map(
        step,
        mesh=mesh,
        in_specs=placed,
        out_specs=(P(None, None, "shard"), P(None, None, "shard"), P("shard", None, None)),
        check_vma=False,
    )
```
